512 devices in a mesh: groups: 2 (over y), wide: 128 (over x, z), narrow: 2 (over core).
Axes of the slice: x: 8, y: 2, z: 16, core: 2. Of those that a mesh axis runs over, the one named last changes fastest.
The devices are a block of a 8x8x16 slice.
Arguments:
- hidden_in: bfloat16 [102400, 1024], P(('groups', 'wide')), parts along dimension 0, may hold values from -6 to 6
- ffn_gain: bfloat16 [1024], replicated, may hold values from 0.5 to 1.5
- wi_gate: bfloat16 [1024, 2816], P('wide', 'narrow'), may hold values from -0.1875 to 0.1875
- wi_up: bfloat16 [1024, 2816], P('wide', 'narrow'), may hold values from -0.1875 to 0.1875
- wo_down: bfloat16 [2816, 1024], P('narrow', 'wide'), may hold values from -0.109375 to 0.109375
- final_gain: bfloat16 [1024], replicated, may hold values from 0.5 to 1.5
- key_w: bfloat16 [1024, 1024], P('wide', 'narrow'), may hold values from -0.1875 to 0.1875
- value_w: bfloat16 [1024, 1024], P('wide', 'narrow'), may hold values from -0.1875 to 0.1875
- query_w: bfloat16 [1024, 1024], P('wide', 'narrow'), may hold values from -8 to 8
- out_w: bfloat16 [1024, 1024], P('narrow', 'wide'), may hold values from -0.1875 to 0.1875
- dec_gain: bfloat16 [1024], replicated, may hold values from 0.5 to 1.5
- embed: bfloat16 [32128, 1024], P('wide'), may hold values from -6 to 6
- lengths: int32 [512], P(('groups', 'wide')), parts along dimension 0, may hold values from 40 to 200
- answer_ids: int32 [8, 32], P('groups'), parts along dimension 0, may hold values from 0 to 32127
Outputs:
- memory: bfloat16 [102400, 1024], P(('groups', 'wide')), parts along dimension 0
- decoded: bfloat16 [256, 1024], P('groups', 'narrow'), parts along dimension 0
The draws below stay inside these ranges and needn't reach their ends.
There are 2 independent parts, one for each index of `groups`. The reference program is written for one: setup_inputs(seed, part) draws one part's arguments, and reference() takes and returns one part's arrays. A program takes and returns all parts, laid end to end along the dimension named above; an argument that names none is the same for every part. Nothing has to cross between parts.
All inputs are finite; a program needn't handle non-finite values.
Results may differ from the reference program's by a relative error of at most 0.0095.
The reference program's roundings to bfloat16 on the way (of `enc_in`, `inner`, `embedded`, `dec_in`, `query` and `attended`) count: a program that leaves them out, or rounds other values in their place, can miss the bound.
Values may be sent and summed in bfloat16 or wider, within the bound.
A program may use at most 64 MiB of HBM per device.

```python
import math
import jax
import jax.numpy as jnp
from jax import lax

D = 1024
HEADS = 16
HEAD_DIM = 64
FF = 2816
VOCAB = 32128
SEG = 200
QUEST = 4
ANS = 32
PASSAGES = 256
TOKENS = 51200
PER_Q = 64
QROWS = 128


def draw_query_w(key, part):
    base = jax.random.normal(jax.random.fold_in(key, 11), (D, D), jnp.float32)
    picked = jax.random.permutation(jax.random.fold_in(key, 12), HEADS)[:2]
    column_head = jnp.arange(D, dtype=jnp.int32) // HEAD_DIM
    strengths = jnp.array([60.0, 100.0], jnp.float32)
    factor = jnp.ones((D,), jnp.float32)
    factor = jnp.where(column_head == picked[0], strengths[0], factor)
    factor = jnp.where(column_head == picked[1], strengths[1], factor)
    scaled = base * (factor / math.sqrt(D))[None, :]
    return jnp.clip(scaled, -8.0, 8.0).astype(jnp.bfloat16)


def set_ends(result, own_key, least, largest):
    place = [jax.random.randint(jax.random.fold_in(own_key, axis), (), 0, length) for axis, length in enumerate(result.shape)]
    longest = result.shape.index(max(result.shape))
    neighbour = place[:longest] + [(place[longest] + 1) % result.shape[longest]] + place[longest + 1:]
    return result.at[tuple(place)].set(least).at[tuple(neighbour)].set(largest)


def shard_levels(rng, shape, split, low, top_value):
    factor_of, own = 1.0, jax.random.fold_in(rng, 6)
    for axis_at, shards_of in split:
        heights = jnp.exp(jax.random.uniform(jax.random.fold_in(own, axis_at), (shards_of,), jnp.float32, low / len(split), top_value / len(split)))
        factor_of = factor_of * jnp.repeat(heights, shape[axis_at] // shards_of).reshape([-1 if axis == axis_at else 1 for axis in range(len(shape))])
    return factor_of


def normal_values(own_key, dims, width, reach, shards=(), kind=jnp.bfloat16):
    drawn = width * jax.random.normal(own_key, dims, jnp.float32)
    if shards:
        drawn = drawn * shard_levels(own_key, dims, shards, -0.22, 0.18)
    return jnp.clip(drawn, -reach, reach).astype(kind)


def setup_inputs(seed: int = 0, part: int = 0) -> dict:
    splits = jax.random.split(jax.random.key(seed), 15)
    part_keys = jax.random.split(jax.random.fold_in(splits[14], part), 15)
    return {
        "hidden_in": normal_values(part_keys[0], (TOKENS, D), 1.0, 6.0, ((0, 128),)),
        "ffn_gain": jnp.clip(1.0 + 0.1 * jax.random.normal(splits[1], (D,), jnp.float32), 0.5, 1.5).astype(jnp.bfloat16),
        "wi_gate": normal_values(splits[2], (D, FF), D ** -0.5, 0.1875, ((0, 128), (1, 2))),
        "wi_up": normal_values(splits[3], (D, FF), D ** -0.5, 0.1875, ((0, 128), (1, 2))),
        "wo_down": normal_values(splits[4], (FF, D), FF ** -0.5, 0.109375, ((0, 2), (1, 128))),
        "final_gain": jnp.clip(1.0 + 0.1 * jax.random.normal(splits[5], (D,), jnp.float32), 0.5, 1.5).astype(jnp.bfloat16),
        "key_w": normal_values(splits[6], (D, D), D ** -0.5, 0.1875, ((0, 128), (1, 2))),
        "value_w": normal_values(splits[7], (D, D), D ** -0.5, 0.1875, ((0, 128), (1, 2))),
        "query_w": draw_query_w(jax.random.fold_in(splits[14], 71), part),
        "out_w": normal_values(splits[9], (D, D), D ** -0.5, 0.1875, ((0, 2), (1, 128))),
        "dec_gain": jnp.clip(1.0 + 0.1 * jax.random.normal(splits[10], (D,), jnp.float32), 0.5, 1.5).astype(jnp.bfloat16),
        "embed": normal_values(splits[11], (VOCAB, D), 1.0, 6.0, ((0, 128),)),
        "lengths": set_ends(jax.random.randint(part_keys[12], (PASSAGES,), SEG // 5, SEG + 1), jax.random.fold_in(part_keys[12], 1), SEG // 5, SEG).astype(jnp.int32),
        "answer_ids": set_ends(jax.random.randint(part_keys[13], (QUEST, ANS), 0, VOCAB), jax.random.fold_in(part_keys[13], 1), 0, VOCAB - 1).astype(jnp.int32),
    }


EPS = 1e-06
FLOOR = -1e+30

def rms_scale(values, gain):
    mean_square = lax.optimization_barrier(jnp.mean(values * values, axis=-1, keepdims=True))
    return values * lax.rsqrt(mean_square + EPS) * gain.astype(jnp.float32)

def reference(hidden_in, ffn_gain, wi_gate, wi_up, wo_down, final_gain, key_w, value_w, query_w, out_w, dec_gain, embed, lengths, answer_ids):

    def encode(block):
        resid_in = block.astype(jnp.float32)
        enc_in = rms_scale(resid_in, ffn_gain).astype(jnp.bfloat16)
        gate = jnp.dot(enc_in, wi_gate, preferred_element_type=jnp.float32)
        up = jnp.dot(enc_in, wi_up, preferred_element_type=jnp.float32)
        inner = (jax.nn.gelu(gate, approximate=True) * up).astype(jnp.bfloat16)
        resid = resid_in + jnp.dot(inner, wo_down, preferred_element_type=jnp.float32)
        memory = rms_scale(resid, final_gain).astype(jnp.bfloat16)
        keys = jnp.dot(memory, key_w, preferred_element_type=jnp.float32).astype(jnp.bfloat16)
        values = jnp.dot(memory, value_w, preferred_element_type=jnp.float32).astype(jnp.bfloat16)
        return (memory, keys, values)
    blocks = hidden_in.reshape(PASSAGES, SEG, D)
    memory, keys, values = lax.map(encode, blocks)
    flat_ids = answer_ids.reshape(QROWS)
    embedded = jnp.take(embed, flat_ids, axis=0)
    dec_in = rms_scale(embedded.astype(jnp.float32), dec_gain).astype(jnp.bfloat16)
    query = jnp.dot(dec_in, query_w, preferred_element_type=jnp.float32).astype(jnp.bfloat16)
    query_four = query.reshape(QUEST, ANS, HEADS, HEAD_DIM).astype(jnp.float32)
    keys_four = keys.reshape(QUEST, PER_Q * SEG, HEADS, HEAD_DIM).astype(jnp.float32)
    values_four = values.reshape(QUEST, PER_Q * SEG, HEADS, HEAD_DIM).astype(jnp.float32)
    position = jnp.arange(SEG, dtype=jnp.int32)
    live = (position[None, :] < lengths[:, None]).reshape(QUEST, PER_Q * SEG)
    scores = jnp.einsum('qahd,qkhd->qahk', query_four, keys_four, precision=lax.Precision.HIGHEST) * (1.0 / math.sqrt(HEAD_DIM))
    scores = jnp.where(live[:, None, None, :], scores, FLOOR)
    weights = jax.nn.softmax(scores, axis=-1)
    attended = jnp.einsum('qahk,qkhd->qahd', weights, values_four, precision=lax.Precision.HIGHEST)
    attended = attended.reshape(QROWS, D).astype(jnp.bfloat16)
    decoded = embedded.astype(jnp.float32) + jnp.dot(attended, out_w, preferred_element_type=jnp.float32)
    return (memory.reshape(TOKENS, D), decoded.astype(jnp.bfloat16))
```

```python
import functools
import math

import jax
import jax.numpy as jnp
from jax import lax
from jax.experimental import pallas as pl
from jax.experimental.pallas import tpu as pltpu
from jax.sharding import Mesh
from jax.sharding import PartitionSpec as P

HEAD_DIM = 64
QUEST = 4
WIDE = ("wide_0", "wide_1")
GROUPS_WIDE = ("groups", "wide_0", "wide_1")
X, Z, CORE = "wide_0", "wide_1", "narrow"
NX, NZ = 8, 16
MESH = pl.DeviceIdType.MESH

EPS = 1e-06
FLOOR = -1e30


def rms_scale(values, gain):
    mean_square = jnp.mean(values * values, axis=-1, keepdims=True)
    return values * lax.rsqrt(mean_square + EPS) * gain.astype(jnp.float32)


def turn(i, by, n):
    return lax.rem(i + (by + 2 * n), n)


def greet(peers):
    barrier = pltpu.get_barrier_semaphore()
    for peer in peers:
        pl.semaphore_signal(barrier, inc=1, device_id=peer, device_id_type=MESH)
    pl.semaphore_wait(barrier, len(peers))


def others(axis, n, steps=None):
    me = lax.axis_index(axis)
    return [{axis: turn(me, d, n)} for d in (steps or range(1, n))]


def remote(src, dst, send, recv, peer):
    return pltpu.make_async_remote_copy(
        src_ref=src, dst_ref=dst, send_sem=send, recv_sem=recv, device_id=peer, device_id_type=MESH
    )


def gather_kernel(a_ref, b_ref, fa, fb, a1, a2, b1, b2, sends, local):
    x, z = lax.axis_index(X), lax.axis_index(Z)
    greet(others(X, NX, (1, -1)) + others(Z, NZ, (1, -1)))
    own = [
        pltpu.make_async_copy(a_ref, fa.at[x * NZ + z], local.at[0]),
        pltpu.make_async_copy(b_ref, fb.at[x * NZ + z], local.at[1]),
    ]
    for copy in own:
        copy.start()

    def block_a(first, second):
        return turn(x, second, NX) * NZ + turn(z, first, NZ)

    def block_b(first, second):
        return turn(x, first, NX) * NZ + turn(z, second, NZ)

    plans = []
    for index, (src, full, block, axis1, n1, axis2, n2, sem1, sem2) in enumerate(
        ((a_ref, fa, block_a, Z, NZ, X, NX, a1, a2), (b_ref, fb, block_b, X, NX, Z, NZ, b1, b2))
    ):
        width = src.shape[1]
        half = width // 256 * 128
        cuts = (pl.ds(0, half), pl.ds(half, width - half))
        me1, me2 = lax.axis_index(axis1), lax.axis_index(axis2)
        peers1 = tuple({axis1: turn(me1, d, n1)} for d in (1, -1))
        peers2 = tuple({axis2: turn(me2, d, n2)} for d in (1, -1))
        plans.append((index, src, full, block, n1, n2, sem1, sem2, cuts, peers1, peers2))

    def off(k):
        odd = lax.rem(k, 2)
        return (1 - odd) * (k // 2) - odd * ((k + 1) // 2)

    def first_stage(plan, t):
        index, src, full, block, n1, n2, sem1, sem2, cuts, peers1, peers2 = plan
        send = sends.at[3 * index]

        @pl.when(t == 0)
        def _():
            mine = full.at[block(0, 0)]
            for d in range(2):
                remote(src, mine, send, sem1.at[1 + d], peers1[d]).start()
            for d in range(2):
                remote(src, mine, send, sem2.at[d, 0, 0], peers2[d]).start()

        @pl.when((t > 0) & (t < n1))
        def _():
            at = full.at[block(off(t), 0)]
            remote(at, at, send, sem1.at[t], peers1[0]).wait_recv()
            odd = lax.rem(t, 2)

            @pl.when((odd == 1) & (t < n1 - 1))
            def _():
                remote(at, at, send, sem1.at[t + 2], peers1[0]).start()

            @pl.when((odd == 0) & (t < n1 - 2))
            def _():
                remote(at, at, send, sem1.at[t + 2], peers1[1]).start()

            for d in range(2):
                remote(at, at, send, sem2.at[d, 0, t], peers2[d]).start()

    def later_stage(plan, t, h):
        index, src, full, block, n1, n2, sem1, sem2, cuts, peers1, peers2 = plan
        last = n2 // 2
        k = t - 2 * h

        @pl.when((k >= 0) & (k < n1))
        def _():
            for d in range(2):
                at = full.at[block(off(k), -h if d == 0 else h)]
                if h == last:
                    part = at.at[:, cuts[d]]
                    remote(
                        part, part, sends.at[3 * index + 1 + d], sem2.at[d, h - 1, k], peers2[d]
                    ).wait_recv()
                    continue
                remote(at, at, sends.at[3 * index], sem2.at[d, h - 1, k], peers2[d]).wait_recv()
                if h + 1 == last:
                    part = at.at[:, cuts[d]]
                    remote(
                        part, part, sends.at[3 * index + 1 + d], sem2.at[d, h, k], peers2[d]
                    ).start()
                else:
                    remote(at, at, sends.at[3 * index], sem2.at[d, h, k], peers2[d]).start()

    def tick(t, carry):
        for plan in plans:
            first_stage(plan, t)
        for h in range(1, max(NX, NZ) // 2 + 1):
            for plan in plans:
                if h <= plan[5] // 2:
                    later_stage(plan, t, h)
        return carry

    lax.fori_loop(0, NX + NZ, tick, 0)
    for copy in own:
        copy.wait()
    for index, src, full, block, n1, n2, sem1, sem2, cuts, peers1, peers2 in plans:
        count = (n1 - 1) + 2 * n1 * (n2 // 2 - 1)
        whole = full.at[pl.ds(0, count)]
        remote(whole, whole, sends.at[3 * index], sem1.at[0], peers1[0]).wait_send()
        for d in range(2):
            part = full.at[pl.ds(0, n1), :, cuts[d]]
            remote(part, part, sends.at[3 * index + 1 + d], sem1.at[0], peers1[0]).wait_send()


def gather_all(a, b):
    n = NX * NZ
    dma = pltpu.SemaphoreType.DMA
    return pl.pallas_call(
        gather_kernel,
        out_shape=(
            jax.ShapeDtypeStruct((n, *a.shape), a.dtype),
            jax.ShapeDtypeStruct((n, *b.shape), b.dtype),
        ),
        in_specs=[pl.BlockSpec(memory_space=pltpu.VMEM)] * 2,
        out_specs=(pl.BlockSpec(memory_space=pl.ANY),) * 2,
        scratch_shapes=[
            dma((NZ,)),
            dma((2, NX // 2, NZ)),
            dma((NX,)),
            dma((2, NZ // 2, NX)),
            dma((6,)),
            dma((2,)),
        ],
        compiler_params=pltpu.CompilerParams(collective_id=1, has_side_effects=True),
        name="gather_weights",
    )(a, b)


def embed_kernel(part, out, got1, s2, got2, s3, got3, send, r1, r2, r3, core_sem):
    x, z, n = lax.axis_index(X), lax.axis_index(Z), lax.axis_index(CORE)
    greet(others(X, NX) + others(Z, NZ) + [{CORE: 1 - n}])
    copies = []
    for d in range(1, NZ):
        to = turn(z, d, NZ)
        copy = remote(part.at[to], got1.at[d], send.at[d], r1.at[d], {Z: to})
        copy.start()
        copies.append(copy)
    total = part[z].astype(jnp.float32)
    for d, copy in enumerate(copies, 1):
        copy.wait_recv()
        total = total + got1[d].astype(jnp.float32)
    for copy in copies:
        copy.wait_send()
    for q in range(QUEST):
        s2[q] = total[2 * q : 2 * q + 2]
    copies = []
    for d in range(1, NX):
        to = turn(x, d, NX)
        copy = remote(s2.at[to // 2], got2.at[d], send.at[d], r2.at[d], {X: to})
        copy.start()
        copies.append(copy)
    total = s2[x // 2]
    for d, copy in enumerate(copies, 1):
        copy.wait_recv()
        total = total + got2[d]
    for copy in copies:
        copy.wait_send()
    s3[...] = total
    got3[z] = total
    copies = []
    for d in range(1, NZ):
        copy = remote(s3, got3.at[z], send.at[d], r3.at[d], {Z: turn(z, d, NZ)})
        copy.start()
        copies.append(copy)
    for d in range(1, NZ):
        slot = got3.at[turn(z, -d, NZ)]
        remote(slot, slot, send.at[d], r3.at[d], {Z: turn(z, d, NZ)}).wait_recv()
    for copy in copies:
        copy.wait_send()
    copy = remote(got3, out.at[n], send.at[0], core_sem.at[0], {CORE: 1 - n})
    copy.start()
    out[n] = got3[...]
    other = out.at[1 - n]
    remote(other, other, send.at[0], core_sem.at[0], {CORE: 1 - n}).wait_recv()
    copy.wait_send()


def embed_rows(part):
    dma = pltpu.SemaphoreType.DMA
    half = part.shape[2]
    return pl.pallas_call(
        embed_kernel,
        out_shape=jax.ShapeDtypeStruct((2, NZ, 2, half), jnp.float32),
        in_specs=[pl.BlockSpec(memory_space=pltpu.VMEM)],
        out_specs=pl.BlockSpec(memory_space=pltpu.VMEM),
        scratch_shapes=[
            pltpu.VMEM(part.shape, part.dtype),
            pltpu.VMEM((QUEST, 2, half), jnp.float32),
            pltpu.VMEM((NX, 2, half), jnp.float32),
            pltpu.VMEM((2, half), jnp.float32),
            pltpu.VMEM((NZ, 2, half), jnp.float32),
            dma((NZ,)),
            dma((NZ,)),
            dma((NX,)),
            dma((NZ,)),
            dma((1,)),
        ],
        compiler_params=pltpu.CompilerParams(collective_id=2, has_side_effects=True),
        name="embed_rows",
    )(part)


def join(parts):
    top = functools.reduce(jnp.maximum, [lse for _, lse in parts])
    weight, total = 0.0, 0.0
    for value, lse in parts:
        factor = jnp.exp(lse - top)
        weight = weight + factor
        total = total + factor * value
    return total / weight, top + jnp.log(weight)


def finish_kernel(
    part, emb, out_w, out, got1, s2, got2, s3, got3, wide, s4, got4, send, r1, r2, r3, r4, r5
):
    x, z, n = lax.axis_index(X), lax.axis_index(Z), lax.axis_index(CORE)
    mate = x + 1 - 2 * lax.rem(x, 2)
    greet(others(Z, NZ) + others(X, NX, (2, 4, 6)) + [{X: mate}, {CORE: 1 - n}])
    copies = []
    for d in range(1, NZ):
        to = turn(z, d, NZ)
        copy = remote(part.at[to], got1.at[d], send.at[d], r1.at[d], {Z: to})
        copy.start()
        copies.append(copy)
    parts = [(part[z, 0], part[z, 1])]
    for d, copy in enumerate(copies, 1):
        copy.wait_recv()
        parts.append((got1[d, 0], got1[d, 1]))
    for copy in copies:
        copy.wait_send()
    value, lse = join(parts)
    s2[0] = value
    s2[1] = lse
    copy = remote(s2, got2, send.at[0], r2.at[0], {X: mate})
    copy.start()
    copy.wait()
    value, _ = join([(value, lse), (got2[0], got2[1])])
    wide[...] = value
    slices = value.shape[0] // 2
    summed = 0.0
    for r in range(slices):
        lhs = wide[2 * r : 2 * r + 2].astype(jnp.bfloat16)
        summed = summed + lax.dot_general(
            lhs,
            out_w[:, 128 * r : 128 * (r + 1)],
            (((1,), (1,)), ((), ())),
            preferred_element_type=jnp.float32,
        )
    half = summed.shape[1] // 2
    s3[0] = summed[:, :half]
    s3[1] = summed[:, half:]
    copy = remote(s3.at[1 - n], got3, send.at[0], r3.at[0], {CORE: 1 - n})
    copy.start()
    copy.wait()
    result = emb[n, z] + (s3[n] + got3[...])
    for r in range(slices):
        wide[2 * r : 2 * r + 2] = result[:, 128 * r : 128 * (r + 1)]
    rows = wide[...].astype(jnp.bfloat16)
    s4[...] = rows
    got4[x // 2] = rows
    copies = []
    for d in (2, 4, 6):
        copy = remote(s4, got4.at[x // 2], send.at[d], r4.at[d], {X: turn(x, d, NX)})
        copy.start()
        copies.append(copy)
    for d in (2, 4, 6):
        slot = got4.at[turn(x, -d, NX) // 2]
        remote(slot, slot, send.at[d], r4.at[d], {X: turn(x, d, NX)}).wait_recv()
    for copy in copies:
        copy.wait_send()
    copies = []
    for d in range(1, NZ):
        copy = remote(got4, out.at[z], send.at[d], r5.at[d], {Z: turn(z, d, NZ)})
        copy.start()
        copies.append(copy)
    out[z] = got4[...]
    for d in range(1, NZ):
        slot = out.at[turn(z, -d, NZ)]
        remote(slot, slot, send.at[d], r5.at[d], {Z: turn(z, d, NZ)}).wait_recv()
    for copy in copies:
        copy.wait_send()


def finish(part, emb, out_w):
    dma = pltpu.SemaphoreType.DMA
    f32 = jnp.float32
    half = emb.shape[3]
    return pl.pallas_call(
        finish_kernel,
        out_shape=jax.ShapeDtypeStruct((NZ, QUEST, 8, 128), jnp.bfloat16),
        in_specs=[pl.BlockSpec(memory_space=pltpu.VMEM)] * 3,
        out_specs=pl.BlockSpec(memory_space=pltpu.VMEM),
        scratch_shapes=[
            pltpu.VMEM(part.shape, f32),
            pltpu.VMEM(part.shape[1:], f32),
            pltpu.VMEM(part.shape[1:], f32),
            pltpu.VMEM((2, 2, half), f32),
            pltpu.VMEM((2, half), f32),
            pltpu.VMEM((8, 128), f32),
            pltpu.VMEM((8, 128), jnp.bfloat16),
            pltpu.VMEM((QUEST, 8, 128), jnp.bfloat16),
            dma((NZ,)),
            dma((NZ,)),
            dma((1,)),
            dma((1,)),
            dma((NX,)),
            dma((NZ,)),
        ],
        compiler_params=pltpu.CompilerParams(collective_id=3, has_side_effects=True),
        name="finish",
    )(part, emb, out_w)


def over_copies(x, axis):
    copies = jnp.broadcast_to(x, (lax.axis_size(axis), *x.shape))
    return lax.all_to_all(copies, axis, split_axis=0, concat_axis=0, tiled=True).sum(axis=0)


def per_device(
    hidden_in,
    ffn_gain,
    wi_gate,
    wi_up,
    wo_down,
    final_gain,
    key_w,
    value_w,
    query_w,
    out_w,
    dec_gain,
    embed,
    lengths,
    answer_ids,
):
    rows = hidden_in.shape[0]
    f32 = jnp.float32
    answers = answer_ids.shape[1]
    vocab_rows, width = embed.shape
    half = width // 2
    ids = answer_ids.reshape(NX, NZ).T.reshape(-1) - lax.axis_index(WIDE) * vocab_rows
    onehot = (ids[:, None] == jnp.arange(vocab_rows, dtype=jnp.int32)[None, :]).astype(jnp.bfloat16)
    table = lax.dynamic_slice_in_dim(embed, lax.axis_index(CORE) * half, half, 1)
    picks = jnp.dot(onehot, table, preferred_element_type=f32).astype(jnp.bfloat16)
    emb = embed_rows(picks.reshape(NZ, NX, half))
    own = emb.transpose(2, 1, 0, 3).reshape(answers, width)
    dec_in = rms_scale(own, dec_gain).astype(jnp.bfloat16)

    ff, proj = wi_gate.shape[1], key_w.shape[1]
    a = jnp.concatenate((wo_down.T, key_w, value_w, query_w, out_w.T), axis=1)
    b = jnp.concatenate((wi_gate, wi_up), axis=1)
    fa, fb = gather_all(a, b)
    fa = fa.reshape(width, a.shape[1])
    fb = fb.reshape(width, b.shape[1])
    down_t, key_full, value_full, query_full, out_t = jnp.split(
        fa, (ff, ff + proj, ff + 2 * proj, ff + 3 * proj), axis=1
    )

    resid_in = hidden_in.astype(f32)
    enc_in = rms_scale(resid_in, ffn_gain).astype(jnp.bfloat16)
    gate = jnp.dot(enc_in, fb[:, :ff], preferred_element_type=f32)
    up = jnp.dot(enc_in, fb[:, ff:], preferred_element_type=f32)
    inner = (jax.nn.gelu(gate, approximate=True) * up).astype(jnp.bfloat16)
    partial_down = lax.dot_general(
        inner, down_t, (((1,), (1,)), ((), ())), preferred_element_type=f32
    )
    resid = resid_in + over_copies(partial_down, CORE)
    memory = rms_scale(resid, final_gain).astype(jnp.bfloat16)

    keys = jnp.dot(memory, key_full, preferred_element_type=f32).astype(jnp.bfloat16)
    values = jnp.dot(memory, value_full, preferred_element_type=f32).astype(jnp.bfloat16)
    query = jnp.dot(dec_in, query_full, preferred_element_type=f32).astype(jnp.bfloat16)
    heads_local = proj // HEAD_DIM
    query_three = query.reshape(answers, heads_local, HEAD_DIM)
    keys_three = keys.reshape(rows, heads_local, HEAD_DIM)
    values_three = values.reshape(rows, heads_local, HEAD_DIM).astype(f32)
    scores = jnp.einsum(
        "ahd,khd->ahk", query_three, keys_three, preferred_element_type=f32
    ) * (1.0 / math.sqrt(HEAD_DIM))
    pass_dev = lengths.shape[0]
    passage_len = rows // pass_dev
    live = (jnp.arange(passage_len, dtype=jnp.int32)[None, :] < lengths[:, None]).reshape(rows)
    scores = jnp.where(live[None, None, :], scores, FLOOR)
    top = jnp.max(scores, axis=2)
    weights = jnp.exp(scores - top[:, :, None])
    total = jnp.sum(weights, axis=2)
    acc = jnp.einsum("ahk,khd->ahd", weights, values_three) / total[:, :, None]
    lse = jnp.broadcast_to((top + jnp.log(total))[:, :, None], acc.shape)
    both = jnp.stack((acc.reshape(answers, proj), lse.reshape(answers, proj)))
    both = both.reshape(2, 2, NZ, proj // 128, 128).transpose(2, 0, 3, 1, 4)
    rows_out = finish(both.reshape(NZ, 2, -1, 128), emb, out_t)
    rows_out = rows_out.reshape(NZ, QUEST, -1, 2, 128).transpose(1, 3, 0, 2, 4)
    return memory, rows_out.reshape(QUEST * answers, half)


def solution(mesh):
    torus = Mesh(
        mesh.devices.reshape(mesh.shape["groups"], NX, NZ, mesh.shape["narrow"]),
        ("groups", "wide_0", "wide_1", "narrow"),
    )
    return jax.shard_map(
        per_device,
        mesh=torus,
        in_specs=(
            P(GROUPS_WIDE, None),
            P(),
            P(WIDE, "narrow"),
            P(WIDE, "narrow"),
            P("narrow", WIDE),
            P(),
            P(WIDE, "narrow"),
            P(WIDE, "narrow"),
            P(WIDE, "narrow"),
            P("narrow", WIDE),
            P(),
            P(WIDE, None),
            P(GROUPS_WIDE),
            P("groups", None),
        ),
        out_specs=(P(GROUPS_WIDE, None), P("groups", "narrow")),
        check_vma=False,
    )
```

```python
import functools
import math

import jax
import jax.numpy as jnp
from jax import lax
from jax.experimental import pallas as pl
from jax.experimental.pallas import tpu as pltpu
from jax.sharding import Mesh
from jax.sharding import PartitionSpec as P

HEAD_DIM = 64
QUEST = 4
WIDE = ("wide_0", "wide_1")
GROUPS_WIDE = ("groups", "wide_0", "wide_1")
X, Z, CORE = "wide_0", "wide_1", "narrow"
NX, NZ = 8, 16
MESH = pl.DeviceIdType.MESH

EPS = 1e-06
FLOOR = -1e30


def turn(i, by, n):
    return lax.rem(i + (by + 2 * n), n)


def others(axis, n, steps=None):
    me = lax.axis_index(axis)
    return [{axis: turn(me, d, n)} for d in (steps or range(1, n))]


def remote(src, dst, send, recv, peer):
    return pltpu.make_async_remote_copy(
        src_ref=src, dst_ref=dst, send_sem=send, recv_sem=recv, device_id=peer, device_id_type=MESH
    )


def join(parts):
    top = functools.reduce(jnp.maximum, [lse for _, lse in parts])
    weight, total = 0.0, 0.0
    for value, lse in parts:
        factor = jnp.exp(lse - top)
        weight = weight + factor
        total = total + factor * value
    return total / weight, top + jnp.log(weight)


def dot(a, b, transposed=False):
    return lax.dot_general(
        a, b, (((1,), (1 if transposed else 0,)), ((), ())), preferred_element_type=jnp.float32
    )


def rows_of(index, count):
    return pl.ds(pl.multiple_of(index * count, count), count)


def reader_kernel(
    hidden,
    gains,
    gate_w,
    up_w,
    down_w,
    key_w,
    value_w,
    query_w,
    out_w,
    table,
    ids,
    lengths,
    memory,
    decoded,
    a_own,
    b_own,
    fa,
    fb,
    enc,
    inner,
    down_mine,
    down_other,
    picks,
    e1,
    e2_src,
    e2,
    e3_src,
    e3,
    emb,
    own_rows,
    part,
    f1,
    f2_src,
    f2,
    wide,
    f3_src,
    f3,
    f4_src,
    f4,
    f5,
    flat,
    a1,
    a2,
    b1,
    b2,
    sends,
    down_send,
    down_recv,
    e_send,
    e_r1,
    e_r2,
    e_r3,
    e_r4,
    f_send,
    f_r1,
    f_r2,
    f_r3,
    f_r4,
    f_r5,
):
    f32, bf16 = jnp.float32, jnp.bfloat16
    x, z, n = lax.axis_index(X), lax.axis_index(Z), lax.axis_index(CORE)
    core = {CORE: 1 - n}
    mate = x + 1 - 2 * lax.rem(x, 2)
    peers = others(X, NX) + others(Z, NZ) + [core]
    barrier = pltpu.get_barrier_semaphore()
    for peer in peers:
        pl.semaphore_signal(barrier, inc=1, device_id=peer, device_id_type=MESH)

    ff, proj = gate_w.shape[1], key_w.shape[1]
    width = hidden.shape[1]
    half = width // 2
    rows = hidden.shape[0]
    answers = own_rows.shape[0]
    at = 0
    for ref in (down_w, key_w, value_w, query_w, out_w):
        a_own[:, at : at + ref.shape[1]] = ref[...]
        at += ref.shape[1]
    for c in range(ff // 128):
        b_own[:, 256 * c : 256 * c + 128] = gate_w[:, 128 * c : 128 * (c + 1)]
        b_own[:, 256 * c + 128 : 256 * (c + 1)] = up_w[:, 128 * c : 128 * (c + 1)]

    vocab_rows = table.shape[0]
    local_ids = ids[...] - (x * NZ + z) * vocab_rows
    spot = lax.broadcasted_iota(jnp.int32, (vocab_rows, ids.shape[1]), 0)
    onehot = (spot == local_ids).astype(f32).astype(bf16)
    shares = lax.dot_general(
        onehot,
        table[:, rows_of(n, half)],
        (((0,), (0,)), ((), ())),
        preferred_element_type=f32,
    ).astype(bf16)
    for k in range(NZ):
        picks[k] = shares[NX * k : NX * (k + 1)]
    pl.semaphore_wait(barrier, len(peers))

    def block_a(first, second):
        return turn(x, second, NX) * NZ + turn(z, first, NZ)

    def block_b(first, second):
        return turn(x, first, NX) * NZ + turn(z, second, NZ)

    plans = []
    for index, (src, full, block, axis1, n1, axis2, n2, sem1, sem2) in enumerate(
        ((a_own, fa, block_a, Z, NZ, X, NX, a1, a2), (b_own, fb, block_b, X, NX, Z, NZ, b1, b2))
    ):
        columns = src.shape[1]
        middle = columns // 256 * 128
        cuts = (pl.ds(0, middle), pl.ds(middle, columns - middle))
        me1, me2 = lax.axis_index(axis1), lax.axis_index(axis2)
        peers1 = tuple({axis1: turn(me1, d, n1)} for d in (1, -1))
        peers2 = tuple({axis2: turn(me2, d, n2)} for d in (1, -1))
        plans.append((index, src, full, block, n1, n2, sem1, sem2, cuts, peers1, peers2))

    def off(k):
        odd = lax.rem(k, 2)
        return (1 - odd) * (k // 2) - odd * ((k + 1) // 2)

    def first_stage(plan, t):
        index, src, full, block, n1, n2, sem1, sem2, cuts, peers1, peers2 = plan
        send = sends.at[3 * index]

        @pl.when(t == 0)
        def _():
            mine = full.at[block(0, 0)]
            for d in range(2):
                remote(src, mine, send, sem1.at[1 + d], peers1[d]).start()
            for d in range(2):
                remote(src, mine, send, sem2.at[d, 0, 0], peers2[d]).start()

        @pl.when((t > 0) & (t < n1))
        def _():
            at = full.at[block(off(t), 0)]
            remote(at, at, send, sem1.at[t], peers1[0]).wait_recv()
            odd = lax.rem(t, 2)

            @pl.when((odd == 1) & (t < n1 - 1))
            def _():
                remote(at, at, send, sem1.at[t + 2], peers1[0]).start()

            @pl.when((odd == 0) & (t < n1 - 2))
            def _():
                remote(at, at, send, sem1.at[t + 2], peers1[1]).start()

            for d in range(2):
                remote(at, at, send, sem2.at[d, 0, t], peers2[d]).start()

    def later_stage(plan, t, h):
        index, src, full, block, n1, n2, sem1, sem2, cuts, peers1, peers2 = plan
        last = n2 // 2
        k = t - 2 * h

        @pl.when((k >= 0) & (k < n1))
        def _():
            for d in range(2):
                at = full.at[block(off(k), -h if d == 0 else h)]
                if h == last:
                    part = at.at[:, cuts[d]]
                    remote(
                        part, part, sends.at[3 * index + 1 + d], sem2.at[d, h - 1, k], peers2[d]
                    ).wait_recv()
                    continue
                remote(at, at, sends.at[3 * index], sem2.at[d, h - 1, k], peers2[d]).wait_recv()
                if h + 1 == last:
                    part = at.at[:, cuts[d]]
                    remote(
                        part, part, sends.at[3 * index + 1 + d], sem2.at[d, h, k], peers2[d]
                    ).start()
                else:
                    remote(at, at, sends.at[3 * index], sem2.at[d, h, k], peers2[d]).start()

    def tick(t, carry):
        for plan in plans:
            first_stage(plan, t)
        for h in range(1, max(NX, NZ) // 2 + 1):
            for plan in plans:
                if h <= plan[5] // 2:
                    later_stage(plan, t, h)
        return carry

    first_copies = []
    for d in range(1, NZ):
        to = turn(z, d, NZ)
        copy = remote(picks.at[to], e1.at[d], e_send.at[d], e_r1.at[d], {Z: to})
        copy.start()
        first_copies.append(copy)
    lax.fori_loop(0, 2, tick, 0)

    resid_in = hidden[...].astype(f32)
    mean_square = jnp.mean(resid_in * resid_in, axis=-1, keepdims=True)
    enc[...] = (resid_in * lax.rsqrt(mean_square + EPS) * gains[0:1]).astype(bf16)
    fa[x * NZ + z] = a_own[...]
    fb[x * NZ + z] = b_own[...]
    lax.fori_loop(2, 5, tick, 0)

    total = picks[z].astype(f32)
    for d, copy in enumerate(first_copies, 1):
        copy.wait_recv()
        total = total + e1[d].astype(f32)
    for copy in first_copies:
        copy.wait_send()
    for q in range(QUEST):
        for r in range(half // 128):
            e2_src[q, 2 * r : 2 * r + 2] = total[2 * q : 2 * q + 2, 128 * r : 128 * (r + 1)]
    copies = []
    for d in range(1, NX):
        to = turn(x, d, NX)
        copy = remote(e2_src.at[to // 2], e2.at[d], e_send.at[d], e_r2.at[d], {X: to})
        copy.start()
        copies.append(copy)
    lax.fori_loop(5, 8, tick, 0)

    total = e2_src[x // 2]
    for d, copy in enumerate(copies, 1):
        copy.wait_recv()
        total = total + e2[d]
    for copy in copies:
        copy.wait_send()
    e3_src[...] = total
    e3[rows_of(z, 8)] = total
    copies = []
    for d in range(1, NZ):
        copy = remote(
            e3_src, e3.at[rows_of(z, 8)], e_send.at[d], e_r3.at[d], {Z: turn(z, d, NZ)}
        )
        copy.start()
        copies.append(copy)
    lax.fori_loop(8, 12, tick, 0)

    for d in range(1, NZ):
        slot = e3.at[rows_of(turn(z, -d, NZ), 8)]
        remote(slot, slot, e_send.at[d], e_r3.at[d], {Z: turn(z, d, NZ)}).wait_recv()
    for copy in copies:
        copy.wait_send()
    copy = remote(e3, emb.at[rows_of(n, 8 * NZ)], e_send.at[0], e_r4.at[0], core)
    copy.start()
    emb[rows_of(n, 8 * NZ)] = e3[...]
    lax.fori_loop(12, 16, tick, 0)

    slot = emb.at[rows_of(1 - n, 8 * NZ)]
    remote(slot, slot, e_send.at[0], e_r4.at[0], core).wait_recv()
    copy.wait_send()
    for h in range(2):
        for r in range(half // 128):
            for i in range(2):
                own_rows[NZ * i : NZ * (i + 1), half * h + 128 * r : half * h + 128 * (r + 1)] = (
                    emb[pl.ds(8 * NZ * h + 2 * r + i, NZ, stride=8), :]
                )
    embedded = own_rows[...]
    mean_square = jnp.mean(embedded * embedded, axis=-1, keepdims=True)
    dec_in = (embedded * lax.rsqrt(mean_square + EPS) * gains[2:3]).astype(bf16)
    lax.fori_loop(16, NX + NZ, tick, 0)

    for index, src, full, block, n1, n2, sem1, sem2, cuts, peers1, peers2 in plans:
        count = (n1 - 1) + 2 * n1 * (n2 // 2 - 1)
        whole = full.at[pl.ds(0, count)]
        remote(whole, whole, sends.at[3 * index], sem1.at[0], peers1[0]).wait_send()
        for d in range(2):
            piece = full.at[pl.ds(0, n1), :, cuts[d]]
            remote(piece, piece, sends.at[3 * index + 1 + d], sem1.at[0], peers1[0]).wait_send()

    def ffn(c, carry):
        weight = fb[:, :, rows_of(c, 256)].reshape(width, 256)
        both = dot(enc[...], weight)
        value = jax.nn.gelu(both[:, :128], approximate=True) * both[:, 128:]
        inner[:, rows_of(c, 128)] = value.astype(bf16)
        return carry

    lax.fori_loop(0, ff // 128, ffn, 0)
    copies = []
    for c in range(width // 256):
        weight = fa[32 * c : 32 * (c + 1), :, :ff].reshape(256, ff)
        down_mine[c] = dot(inner[...], weight, True)
        copy = remote(down_mine.at[c], down_other.at[c], down_send.at[c], down_recv.at[c], core)
        copy.start()
        copies.append(copy)
    query = dot(dec_in, fa[:, :, ff + 2 * proj : ff + 3 * proj].reshape(width, proj)).astype(bf16)
    squares = 0.0
    for c, copy in enumerate(copies):
        copy.wait_recv()
        resid = hidden[:, 256 * c : 256 * (c + 1)].astype(f32) + (down_mine[c] + down_other[c])
        down_other[c] = resid
        squares = squares + jnp.sum(resid * resid, axis=-1, keepdims=True)
    scale = lax.rsqrt(squares * (1.0 / width) + EPS)
    for c in range(width // 256):
        cols = slice(256 * c, 256 * (c + 1))
        memory[:, cols] = (down_other[c] * scale * gains[1:2, cols]).astype(bf16)
    for copy in copies:
        copy.wait_send()

    mem = memory[...]
    keys = dot(mem, fa[:, :, ff : ff + proj].reshape(width, proj)).astype(bf16)
    values = dot(mem, fa[:, :, ff + proj : ff + 2 * proj].reshape(width, proj)).astype(bf16)
    heads = proj // HEAD_DIM
    head_of = lax.broadcasted_iota(jnp.int32, (answers, proj), 1) // HEAD_DIM
    spread = jnp.concatenate(
        [jnp.where(head_of == h, query.astype(f32), 0.0) for h in range(heads)], axis=0
    ).astype(bf16)
    scores = dot(spread, keys, True) * (1.0 / math.sqrt(HEAD_DIM))
    position = lax.broadcasted_iota(jnp.int32, scores.shape, 1)
    passages = lengths.shape[0]
    passage_len = rows // passages
    live = None
    for p in range(passages):
        here = (position >= p * passage_len) & (position < p * passage_len + lengths[p])
        live = here if live is None else live | here
    scores = jnp.where(live, scores, FLOOR)
    top = jnp.max(scores, axis=1, keepdims=True)
    weights = jnp.exp(scores - top)
    total = jnp.sum(weights, axis=1, keepdims=True)
    acc = dot(weights.astype(bf16), values) / total
    lse = top + jnp.log(total)
    value, spread_lse = 0.0, 0.0
    for h in range(heads):
        rows_h = slice(answers * h, answers * (h + 1))
        value = value + jnp.where(head_of == h, acc[rows_h], 0.0)
        spread_lse = spread_lse + jnp.where(head_of == h, lse[rows_h], 0.0)
    for s, block_of in enumerate((value, spread_lse)):
        for r in range(proj // 128):
            for i in range(2):
                part[pl.ds(8 * s + 2 * r + i, NZ, stride=16), :] = block_of[
                    NZ * i : NZ * (i + 1), 128 * r : 128 * (r + 1)
                ]

    copies = []
    for d in range(1, NZ):
        to = turn(z, d, NZ)
        copy = remote(
            part.at[rows_of(to, 16)], f1.at[d], f_send.at[d], f_r1.at[d], {Z: to}
        )
        copy.start()
        copies.append(copy)
    mine = part[rows_of(z, 16)]
    parts = [(mine[:8], mine[8:])]
    for d, copy in enumerate(copies, 1):
        copy.wait_recv()
        parts.append((f1[d, :8], f1[d, 8:]))
    value, lse = join(parts)
    f2_src[0] = value
    f2_src[1] = lse
    pair = remote(f2_src, f2, f_send.at[0], f_r2.at[0], {X: mate})
    pair.start()
    for copy in copies:
        copy.wait_send()
    pair.wait()
    value, _ = join([(value, lse), (f2[0], f2[1])])
    wide[...] = value
    slices = proj // 128
    summed = 0.0
    for r in range(slices):
        lhs = wide[2 * r : 2 * r + 2].astype(bf16)
        at = ff + 3 * proj + 128 * r
        summed = summed + dot(lhs, fa[:, :, at : at + 128].reshape(width, 128), True)
    for h in range(2):
        for r in range(half // 128):
            at = half * h + 128 * r
            f3_src[h, 2 * r : 2 * r + 2] = summed[:, at : at + 128]
    copy = remote(f3_src.at[1 - n], f3, f_send.at[0], f_r3.at[0], core)
    copy.start()
    copy.wait()
    result = emb[pl.ds(pl.multiple_of(n * 8 * NZ + z * 8, 8), 8)] + (f3_src[n] + f3[...])
    done = result.astype(bf16)
    f4_src[...] = done
    f4[x // 2] = done
    copies = []
    for d in (2, 4, 6):
        copy = remote(f4_src, f4.at[x // 2], f_send.at[d], f_r4.at[d], {X: turn(x, d, NX)})
        copy.start()
        copies.append(copy)
    for d in (2, 4, 6):
        slot = f4.at[turn(x, -d, NX) // 2]
        remote(slot, slot, f_send.at[d], f_r4.at[d], {X: turn(x, d, NX)}).wait_recv()
    for copy in copies:
        copy.wait_send()
    copies = []
    for d in range(1, NZ):
        copy = remote(f4, f5.at[z], f_send.at[d], f_r5.at[d], {Z: turn(z, d, NZ)})
        copy.start()
        copies.append(copy)
    f5[z] = f4[...]
    for d in range(1, NZ):
        slot = f5.at[turn(z, -d, NZ)]
        remote(slot, slot, f_send.at[d], f_r5.at[d], {Z: turn(z, d, NZ)}).wait_recv()
    for k in range(NZ):
        for q in range(QUEST):
            flat[8 * (QUEST * k + q) : 8 * (QUEST * k + q + 1)] = f5[k, q].astype(f32)
    for q in range(QUEST):
        for i in range(2):
            for r in range(half // 128):
                start = NZ * (2 * q + i)
                decoded[start : start + NZ, 128 * r : 128 * (r + 1)] = flat[
                    pl.ds(8 * q + 2 * r + i, NZ, stride=8 * QUEST), :
                ].astype(bf16)
    for copy in copies:
        copy.wait_send()


def reader(hidden, gains, shards, table, ids, lengths, answers):
    gate_w, up_w, down_w, key_w, value_w, query_w, out_w = shards
    dma = pltpu.SemaphoreType.DMA
    f32, bf16 = jnp.float32, jnp.bfloat16
    blocks = NX * NZ
    rows, width = hidden.shape
    ff, proj, half = gate_w.shape[1], key_w.shape[1], width // 2
    a_width, b_width = ff + 4 * proj, 2 * ff
    chunks = width // 256
    vmem = pltpu.VMEM
    scratch = [
        vmem((8, a_width), bf16),
        vmem((8, b_width), bf16),
        vmem((blocks, 8, a_width), bf16),
        vmem((blocks, 8, b_width), bf16),
        vmem((rows, width), bf16),
        vmem((rows, ff), bf16),
        vmem((chunks, rows, 256), f32),
        vmem((chunks, rows, 256), f32),
        vmem((NZ, NX, half), bf16),
        vmem((NZ, NX, half), bf16),
        vmem((QUEST, 8, 128), f32),
        vmem((NX, 8, 128), f32),
        vmem((8, 128), f32),
        vmem((8 * NZ, 128), f32),
        vmem((16 * NZ, 128), f32),
        vmem((answers, width), f32),
        vmem((16 * NZ, 128), f32),
        vmem((NZ, 16, 128), f32),
        vmem((2, 8, 128), f32),
        vmem((2, 8, 128), f32),
        vmem((8, 128), f32),
        vmem((2, 8, 128), f32),
        vmem((8, 128), f32),
        vmem((8, 128), bf16),
        vmem((QUEST, 8, 128), bf16),
        vmem((NZ, QUEST, 8, 128), bf16),
        vmem((NZ * QUEST * 8, 128), f32),
        dma((NZ,)),
        dma((2, NX // 2, NZ)),
        dma((NX,)),
        dma((2, NZ // 2, NX)),
        dma((6,)),
        dma((chunks,)),
        dma((chunks,)),
        dma((NZ,)),
        dma((NZ,)),
        dma((NX,)),
        dma((NZ,)),
        dma((1,)),
        dma((NZ,)),
        dma((NZ,)),
        dma((1,)),
        dma((1,)),
        dma((NX,)),
        dma((NZ,)),
    ]
    return pl.pallas_call(
        reader_kernel,
        out_shape=(
            jax.ShapeDtypeStruct((rows, width), bf16),
            jax.ShapeDtypeStruct((QUEST * answers, half), bf16),
        ),
        in_specs=[pl.BlockSpec(memory_space=vmem)] * 11 + [pl.BlockSpec(memory_space=pltpu.SMEM)],
        out_specs=(pl.BlockSpec(memory_space=vmem),) * 2,
        scratch_shapes=scratch,
        compiler_params=pltpu.CompilerParams(
            collective_id=1, has_side_effects=True, vmem_limit_bytes=60 * 2**20
        ),
        name="reader",
    )(hidden, gains, *shards, table, ids, lengths)


def per_device(
    hidden_in,
    ffn_gain,
    wi_gate,
    wi_up,
    wo_down,
    final_gain,
    key_w,
    value_w,
    query_w,
    out_w,
    dec_gain,
    embed,
    lengths,
    answer_ids,
):
    gains = jnp.stack((ffn_gain, final_gain, dec_gain)).astype(jnp.float32)
    ids = answer_ids.reshape(NX, NZ).T.reshape(1, NX * NZ)
    shards = (wi_gate, wi_up, wo_down.T, key_w, value_w, query_w, out_w.T)
    return reader(hidden_in, gains, shards, embed, ids, lengths, answer_ids.shape[1])


def solution(mesh):
    torus = Mesh(
        mesh.devices.reshape(mesh.shape["groups"], NX, NZ, mesh.shape["narrow"]),
        ("groups", "wide_0", "wide_1", "narrow"),
    )
    return jax.shard_map(
        per_device,
        mesh=torus,
        in_specs=(
            P(GROUPS_WIDE, None),
            P(),
            P(WIDE, "narrow"),
            P(WIDE, "narrow"),
            P("narrow", WIDE),
            P(),
            P(WIDE, "narrow"),
            P(WIDE, "narrow"),
            P(WIDE, "narrow"),
            P("narrow", WIDE),
            P(),
            P(WIDE, None),
            P(GROUPS_WIDE),
            P("groups", None),
        ),
        out_specs=(P(GROUPS_WIDE, None), P("groups", "narrow")),
        check_vma=False,
    )
```

```python
import functools
import math

import jax
import jax.numpy as jnp
from jax import lax
from jax.experimental import pallas as pl
from jax.experimental.pallas import tpu as pltpu
from jax.sharding import Mesh
from jax.sharding import PartitionSpec as P

HEAD_DIM = 64
QUEST = 4
WIDE = ("wide_0", "wide_1")
GROUPS_WIDE = ("groups", "wide_0", "wide_1")
X, Z, CORE = "wide_0", "wide_1", "narrow"
NX, NZ = 8, 16
MESH = pl.DeviceIdType.MESH

EPS = 1e-06
FLOOR = -1e30


def turn(i, by, n):
    return lax.rem(i + (by + 2 * n), n)


def others(axis, n, steps=None):
    me = lax.axis_index(axis)
    return [{axis: turn(me, d, n)} for d in (steps or range(1, n))]


def remote(src, dst, send, recv, peer):
    return pltpu.make_async_remote_copy(
        src_ref=src, dst_ref=dst, send_sem=send, recv_sem=recv, device_id=peer, device_id_type=MESH
    )


def join(parts):
    top = functools.reduce(jnp.maximum, [lse for _, lse in parts])
    weight, total = 0.0, 0.0
    for value, lse in parts:
        factor = jnp.exp(lse - top)
        weight = weight + factor
        total = total + factor * value
    return total / weight, top + jnp.log(weight)


def dot(a, b, transposed=False):
    return lax.dot_general(
        a, b, (((1,), (1 if transposed else 0,)), ((), ())), preferred_element_type=jnp.float32
    )


def gain_of(ref):
    return ref[...].astype(jnp.float32).reshape(1, -1)


def rows_of(index, count):
    return pl.ds(pl.multiple_of(index * count, count), count)


def reader_kernel(
    hidden_in,
    ffn_gain_in,
    final_gain_in,
    dec_gain_in,
    gate_w,
    up_w,
    down_w,
    key_w,
    value_w,
    query_w,
    out_w,
    table_in,
    ids_in,
    lengths,
    memory_out,
    decoded,
    hidden,
    ffn_gain,
    final_gain,
    dec_gain,
    table,
    ids,
    memory,
    spread_picks,
    a_own,
    b_own,
    fa,
    fb,
    enc,
    inner,
    down_mine,
    down_other,
    picks,
    e1,
    e2_src,
    e2,
    e3_src,
    e3,
    emb,
    own_rows,
    part,
    f1,
    f2_src,
    f2,
    wide,
    f3_src,
    f3,
    f4_src,
    f4,
    f5,
    flat,
    load_sem,
    a1,
    a2,
    b1,
    b2,
    sends,
    y_send,
    y_recv,
    down_send,
    down_recv,
    e_send,
    e_r1,
    e_r2,
    e_r3,
    e_r4,
    f_send,
    f_r1,
    f_r2,
    f_r3,
    f_r4,
    f_r5,
):
    f32, bf16 = jnp.float32, jnp.bfloat16
    x, z, n = lax.axis_index(X), lax.axis_index(Z), lax.axis_index(CORE)
    core = {CORE: 1 - n}
    group = lax.axis_index("groups")
    parity = lax.rem(group, 2)
    partner = {"groups": group + 1 - 2 * parity}
    mate = x + 1 - 2 * lax.rem(x, 2)
    ff, proj = gate_w.shape[1], key_w.shape[1]
    width = hidden.shape[1]
    half = width // 2
    rows = hidden.shape[0]
    answers = own_rows.shape[0]
    loads, at = [], 0
    for ref in (down_w, key_w, value_w, query_w, out_w):
        loads.append((ref, a_own.at[:, at : at + ref.shape[1]]))
        at += ref.shape[1]
    loads += [(gate_w, b_own.at[:, :ff]), (up_w, b_own.at[:, ff:])]
    loads += [(ids_in, ids), (table_in.at[:, rows_of(n, half)], table)]
    shard_loads = len(loads)
    loads += [(hidden_in, hidden), (ffn_gain_in, ffn_gain)]
    loads += [(final_gain_in, final_gain), (dec_gain_in, dec_gain)]
    loads = [
        pltpu.make_async_copy(src, dst, load_sem.at[k]) for k, (src, dst) in enumerate(loads)
    ]
    for load in loads:
        load.start()
    peers = others(X, NX) + others(Z, NZ) + [core, partner]
    barrier = pltpu.get_barrier_semaphore()
    for peer in peers:
        pl.semaphore_signal(barrier, inc=1, device_id=peer, device_id_type=MESH)
    for load in loads[:shard_loads]:
        load.wait()

    vocab_rows = table.shape[0]
    spot = lax.broadcasted_iota(jnp.int32, (vocab_rows, answers), 0)
    for q in range(QUEST):
        local_ids = ids[q : q + 1] - (x * NZ + z) * vocab_rows
        shares = lax.dot_general(
            (spot == local_ids).astype(f32).astype(bf16),
            table[...],
            (((0,), (0,)), ((), ())),
            preferred_element_type=f32,
        )
        for i in range(2):
            for r in range(half // 128):
                spread_picks[r, pl.ds(2 * q + i, NZ, stride=NX), :] = shares[
                    NZ * i : NZ * (i + 1), 128 * r : 128 * (r + 1)
                ]
    for k in range(NZ):
        for r in range(half // 128):
            picks[k, :, 128 * r : 128 * (r + 1)] = spread_picks[
                r, NX * k : NX * (k + 1)
            ].astype(bf16)
    pl.semaphore_wait(barrier, len(peers))

    def block_a(first, second):
        return turn(x, second, NX) * NZ + turn(z, first, NZ)

    def block_b(first, second):
        return turn(x, first, NX) * NZ + turn(z, second, NZ)

    plans = []
    for index, (src, full, block, axis1, n1, axis2, n2, sem1, sem2) in enumerate(
        ((a_own, fa, block_a, Z, NZ, X, NX, a1, a2), (b_own, fb, block_b, X, NX, Z, NZ, b1, b2))
    ):
        total = src.shape[1]
        share = total // 128 * 2 // 11 * 128 + (128 if index == 0 else 0)
        columns = total - share
        middle = columns // 256 * 128
        start = parity * share
        cuts = (
            pl.ds(pl.multiple_of(start, 128), middle),
            pl.ds(pl.multiple_of(start + middle, 128), columns - middle),
        )
        area = pl.ds(pl.multiple_of(start, 128), columns)
        given = pl.ds(pl.multiple_of(parity * columns, 128), share)
        me1, me2 = lax.axis_index(axis1), lax.axis_index(axis2)
        peers1 = tuple({axis1: turn(me1, d, n1)} for d in (1, -1))
        peers2 = tuple({axis2: turn(me2, d, n2)} for d in (1, -1))
        plans.append(
            (index, src, full, block, n1, n2, sem1, sem2, cuts, peers1, peers2, area, given)
        )

    def off(k):
        odd = lax.rem(k, 2)
        return (1 - odd) * (k // 2) - odd * ((k + 1) // 2)

    def hand_over(plan, src, which):
        index, full, given = plan[0], plan[2], plan[12]
        remote(
            src.at[:, given], full.at[which, :, given], y_send.at[index], y_recv.at[index], partner
        ).start()

    def first_stage(plan, t):
        index, src, full, block, n1, n2, sem1, sem2, cuts, peers1, peers2, area, given = plan
        send = sends.at[3 * index]

        @pl.when(t == 0)
        def _():
            mine = full.at[block(0, 0), :, area]
            hand_over(plan, src, block(0, 0))
            sent = src.at[:, area]
            for d in range(2):
                remote(sent, mine, send, sem1.at[1 + d], peers1[d]).start()
            for d in range(2):
                remote(sent, mine, send, sem2.at[d, 0, 0], peers2[d]).start()

        @pl.when((t > 0) & (t < n1))
        def _():
            at = full.at[block(off(t), 0), :, area]
            remote(at, at, send, sem1.at[t], peers1[0]).wait_recv()
            odd = lax.rem(t, 2)

            @pl.when((odd == 1) & (t < n1 - 1))
            def _():
                remote(at, at, send, sem1.at[t + 2], peers1[0]).start()

            @pl.when((odd == 0) & (t < n1 - 2))
            def _():
                remote(at, at, send, sem1.at[t + 2], peers1[1]).start()

            for d in range(2):
                remote(at, at, send, sem2.at[d, 0, t], peers2[d]).start()
            hand_over(plan, full.at[block(off(t), 0)], block(off(t), 0))

    def later_stage(plan, t, h):
        index, src, full, block, n1, n2, sem1, sem2, cuts, peers1, peers2, area, given = plan
        last = n2 // 2
        k = t - 2 * h

        @pl.when((k >= 0) & (k < n1))
        def _():
            for d in range(2):
                which = block(off(k), -h if d == 0 else h)
                at = full.at[which, :, area]
                part = full.at[which, :, cuts[d]]
                if h == last:
                    remote(
                        part, part, sends.at[3 * index + 1 + d], sem2.at[d, h - 1, k], peers2[d]
                    ).wait_recv()
                    if d == 1:
                        hand_over(plan, full.at[which], which)
                    continue
                remote(at, at, sends.at[3 * index], sem2.at[d, h - 1, k], peers2[d]).wait_recv()
                if h + 1 == last:
                    remote(
                        part, part, sends.at[3 * index + 1 + d], sem2.at[d, h, k], peers2[d]
                    ).start()
                else:
                    remote(at, at, sends.at[3 * index], sem2.at[d, h, k], peers2[d]).start()
                hand_over(plan, full.at[which], which)

    def tick(t, carry):
        for plan in plans:
            first_stage(plan, t)
        for h in range(1, max(NX, NZ) // 2 + 1):
            for plan in plans:
                if h <= plan[5] // 2:
                    later_stage(plan, t, h)
        return carry

    first_copies = []
    for d in range(1, NZ):
        to = turn(z, d, NZ)
        copy = remote(picks.at[to], e1.at[d], e_send.at[d], e_r1.at[d], {Z: to})
        copy.start()
        first_copies.append(copy)
    lax.fori_loop(0, 2, tick, 0)

    for load in loads[shard_loads:]:
        load.wait()
    resid_in = hidden[...].astype(f32)
    mean_square = jnp.mean(resid_in * resid_in, axis=-1, keepdims=True)
    enc[...] = (resid_in * lax.rsqrt(mean_square + EPS) * gain_of(ffn_gain)).astype(bf16)
    for index, src, full, block, *_, area, given in plans:
        full[block(0, 0), :, area] = src[:, area]
    lax.fori_loop(2, 5, tick, 0)

    total = picks[z].astype(f32)
    for d, copy in enumerate(first_copies, 1):
        copy.wait_recv()
        total = total + e1[d].astype(f32)
    for copy in first_copies:
        copy.wait_send()
    for q in range(QUEST):
        for r in range(half // 128):
            e2_src[q, 2 * r : 2 * r + 2] = total[2 * q : 2 * q + 2, 128 * r : 128 * (r + 1)]
    copies = []
    for d in range(1, NX):
        to = turn(x, d, NX)
        copy = remote(e2_src.at[to // 2], e2.at[d], e_send.at[d], e_r2.at[d], {X: to})
        copy.start()
        copies.append(copy)
    lax.fori_loop(5, 8, tick, 0)

    total = e2_src[x // 2]
    for d, copy in enumerate(copies, 1):
        copy.wait_recv()
        total = total + e2[d]
    for copy in copies:
        copy.wait_send()
    e3_src[...] = total
    e3[rows_of(z, 8)] = total
    copies = []
    for d in range(1, NZ):
        copy = remote(
            e3_src, e3.at[rows_of(z, 8)], e_send.at[d], e_r3.at[d], {Z: turn(z, d, NZ)}
        )
        copy.start()
        copies.append(copy)
    lax.fori_loop(8, 12, tick, 0)

    for d in range(1, NZ):
        slot = e3.at[rows_of(turn(z, -d, NZ), 8)]
        remote(slot, slot, e_send.at[d], e_r3.at[d], {Z: turn(z, d, NZ)}).wait_recv()
    for copy in copies:
        copy.wait_send()
    copy = remote(e3, emb.at[rows_of(n, 8 * NZ)], e_send.at[0], e_r4.at[0], core)
    copy.start()
    emb[rows_of(n, 8 * NZ)] = e3[...]
    lax.fori_loop(12, 16, tick, 0)

    slot = emb.at[rows_of(1 - n, 8 * NZ)]
    remote(slot, slot, e_send.at[0], e_r4.at[0], core).wait_recv()
    copy.wait_send()
    for h in range(2):
        for r in range(half // 128):
            for i in range(2):
                own_rows[NZ * i : NZ * (i + 1), half * h + 128 * r : half * h + 128 * (r + 1)] = (
                    emb[pl.ds(8 * NZ * h + 2 * r + i, NZ, stride=8), :]
                )
    embedded = own_rows[...]
    mean_square = jnp.mean(embedded * embedded, axis=-1, keepdims=True)
    dec_in = (embedded * lax.rsqrt(mean_square + EPS) * gain_of(dec_gain)).astype(bf16)
    lax.fori_loop(16, NX + NZ, tick, 0)

    for index, src, full, block, n1, n2, sem1, sem2, cuts, peers1, peers2, area, given in plans:
        count = (n1 - 1) + 2 * n1 * (n2 // 2 - 1)
        whole = full.at[:, :, given]
        remote(whole, whole, y_send.at[index], y_recv.at[index], partner).wait()
        whole = full.at[pl.ds(0, count), :, area]
        remote(whole, whole, sends.at[3 * index], sem1.at[0], peers1[0]).wait_send()
        for d in range(2):
            piece = full.at[pl.ds(0, n1), :, cuts[d]]
            remote(piece, piece, sends.at[3 * index + 1 + d], sem1.at[0], peers1[0]).wait_send()

    def ffn(c, carry):
        gate_at = pl.ds(pl.multiple_of(c * 128, 128), 128)
        up_at = pl.ds(pl.multiple_of(ff + c * 128, 128), 128)
        weight = jnp.concatenate((fb[:, :, gate_at], fb[:, :, up_at]), axis=2).reshape(width, 256)
        both = dot(enc[...], weight)
        value = jax.nn.gelu(both[:, :128], approximate=True) * both[:, 128:]
        inner[:, rows_of(c, 128)] = value.astype(bf16)
        return carry

    lax.fori_loop(0, ff // 128, ffn, 0)
    copies = []
    for c in range(width // 256):
        weight = fa[32 * c : 32 * (c + 1), :, :ff].reshape(256, ff)
        down_mine[c] = dot(inner[...], weight, True)
        copy = remote(down_mine.at[c], down_other.at[c], down_send.at[c], down_recv.at[c], core)
        copy.start()
        copies.append(copy)
    query = dot(dec_in, fa[:, :, ff + 2 * proj : ff + 3 * proj].reshape(width, proj)).astype(bf16)
    squares = 0.0
    for c, copy in enumerate(copies):
        copy.wait_recv()
        resid = hidden[:, 256 * c : 256 * (c + 1)].astype(f32) + (down_mine[c] + down_other[c])
        down_other[c] = resid
        squares = squares + jnp.sum(resid * resid, axis=-1, keepdims=True)
    scale = lax.rsqrt(squares * (1.0 / width) + EPS)
    gain = gain_of(final_gain)
    for c in range(width // 256):
        cols = slice(256 * c, 256 * (c + 1))
        memory[:, cols] = (down_other[c] * scale * gain[:, cols]).astype(bf16)
    for copy in copies:
        copy.wait_send()
    store = pltpu.make_async_copy(memory, memory_out, load_sem.at[0])
    store.start()

    mem = memory[...]
    keys = dot(mem, fa[:, :, ff : ff + proj].reshape(width, proj)).astype(bf16)
    values = dot(mem, fa[:, :, ff + proj : ff + 2 * proj].reshape(width, proj)).astype(bf16)
    heads = proj // HEAD_DIM
    head_of = lax.broadcasted_iota(jnp.int32, (answers, proj), 1) // HEAD_DIM
    spread = jnp.concatenate(
        [jnp.where(head_of == h, query.astype(f32), 0.0) for h in range(heads)], axis=0
    ).astype(bf16)
    scores = dot(spread, keys, True) * (1.0 / math.sqrt(HEAD_DIM))
    position = lax.broadcasted_iota(jnp.int32, scores.shape, 1)
    passages = lengths.shape[0]
    passage_len = rows // passages
    live = None
    for p in range(passages):
        here = (position >= p * passage_len) & (position < p * passage_len + lengths[p])
        live = here if live is None else live | here
    scores = jnp.where(live, scores, FLOOR)
    top = jnp.max(scores, axis=1, keepdims=True)
    weights = jnp.exp(scores - top)
    total = jnp.sum(weights, axis=1, keepdims=True)
    acc = dot(weights.astype(bf16), values) / total
    lse = top + jnp.log(total)
    value, spread_lse = 0.0, 0.0
    for h in range(heads):
        rows_h = slice(answers * h, answers * (h + 1))
        value = value + jnp.where(head_of == h, acc[rows_h], 0.0)
        spread_lse = spread_lse + jnp.where(head_of == h, lse[rows_h], 0.0)
    for s, block_of in enumerate((value, spread_lse)):
        for r in range(proj // 128):
            for i in range(2):
                part[pl.ds(8 * s + 2 * r + i, NZ, stride=16), :] = block_of[
                    NZ * i : NZ * (i + 1), 128 * r : 128 * (r + 1)
                ]

    copies = []
    for d in range(1, NZ):
        to = turn(z, d, NZ)
        copy = remote(
            part.at[rows_of(to, 16)], f1.at[d], f_send.at[d], f_r1.at[d], {Z: to}
        )
        copy.start()
        copies.append(copy)
    mine = part[rows_of(z, 16)]
    parts = [(mine[:8], mine[8:])]
    for d, copy in enumerate(copies, 1):
        copy.wait_recv()
        parts.append((f1[d, :8], f1[d, 8:]))
    value, lse = join(parts)
    f2_src[0] = value
    f2_src[1] = lse
    pair = remote(f2_src, f2, f_send.at[0], f_r2.at[0], {X: mate})
    pair.start()
    for copy in copies:
        copy.wait_send()
    pair.wait()
    value, _ = join([(value, lse), (f2[0], f2[1])])
    wide[...] = value
    slices = proj // 128
    summed = 0.0
    for r in range(slices):
        lhs = wide[2 * r : 2 * r + 2].astype(bf16)
        at = ff + 3 * proj + 128 * r
        summed = summed + dot(lhs, fa[:, :, at : at + 128].reshape(width, 128), True)
    for h in range(2):
        for r in range(half // 128):
            at = half * h + 128 * r
            f3_src[h, 2 * r : 2 * r + 2] = summed[:, at : at + 128]
    copy = remote(f3_src.at[1 - n], f3, f_send.at[0], f_r3.at[0], core)
    copy.start()
    copy.wait()
    result = emb[pl.ds(pl.multiple_of(n * 8 * NZ + z * 8, 8), 8)] + (f3_src[n] + f3[...])
    done = result.astype(bf16)
    f4_src[...] = done
    f4[x // 2] = done
    copies = []
    for d in (2, 4, 6):
        copy = remote(f4_src, f4.at[x // 2], f_send.at[d], f_r4.at[d], {X: turn(x, d, NX)})
        copy.start()
        copies.append(copy)
    for d in (2, 4, 6):
        slot = f4.at[turn(x, -d, NX) // 2]
        remote(slot, slot, f_send.at[d], f_r4.at[d], {X: turn(x, d, NX)}).wait_recv()
    for copy in copies:
        copy.wait_send()
    copies = []
    for d in range(1, NZ):
        copy = remote(f4, f5.at[z], f_send.at[d], f_r5.at[d], {Z: turn(z, d, NZ)})
        copy.start()
        copies.append(copy)
    f5[z] = f4[...]
    for d in range(1, NZ):
        slot = f5.at[turn(z, -d, NZ)]
        remote(slot, slot, f_send.at[d], f_r5.at[d], {Z: turn(z, d, NZ)}).wait_recv()
    for k in range(NZ):
        for q in range(QUEST):
            flat[8 * (QUEST * k + q) : 8 * (QUEST * k + q + 1)] = f5[k, q].astype(f32)
    for q in range(QUEST):
        for i in range(2):
            for r in range(half // 128):
                start = NZ * (2 * q + i)
                decoded[start : start + NZ, 128 * r : 128 * (r + 1)] = flat[
                    pl.ds(8 * q + 2 * r + i, NZ, stride=8 * QUEST), :
                ].astype(bf16)
    for copy in copies:
        copy.wait_send()
    store.wait()


def reader(hidden, gains, shards, table, ids, lengths):
    gate_w, up_w, down_w, key_w, value_w, query_w, out_w = shards
    dma = pltpu.SemaphoreType.DMA
    f32, bf16 = jnp.float32, jnp.bfloat16
    blocks = NX * NZ
    answers = ids.shape[1]
    rows, width = hidden.shape
    ff, proj, half = gate_w.shape[1], key_w.shape[1], width // 2
    a_width, b_width = ff + 4 * proj, 2 * ff
    chunks = width // 256
    vmem = pltpu.VMEM
    scratch = [
        vmem((rows, width), bf16),
        *[vmem(gain.shape, bf16) for gain in gains],
        vmem((table.shape[0], half), bf16),
        vmem(ids.shape, ids.dtype),
        vmem((rows, width), bf16),
        vmem((half // 128, NX * NZ, 128), f32),
        vmem((8, a_width), bf16),
        vmem((8, b_width), bf16),
        vmem((blocks, 8, a_width), bf16),
        vmem((blocks, 8, b_width), bf16),
        vmem((rows, width), bf16),
        vmem((rows, ff), bf16),
        vmem((chunks, rows, 256), f32),
        vmem((chunks, rows, 256), f32),
        vmem((NZ, NX, half), bf16),
        vmem((NZ, NX, half), bf16),
        vmem((QUEST, 8, 128), f32),
        vmem((NX, 8, 128), f32),
        vmem((8, 128), f32),
        vmem((8 * NZ, 128), f32),
        vmem((16 * NZ, 128), f32),
        vmem((answers, width), f32),
        vmem((16 * NZ, 128), f32),
        vmem((NZ, 16, 128), f32),
        vmem((2, 8, 128), f32),
        vmem((2, 8, 128), f32),
        vmem((8, 128), f32),
        vmem((2, 8, 128), f32),
        vmem((8, 128), f32),
        vmem((8, 128), bf16),
        vmem((QUEST, 8, 128), bf16),
        vmem((NZ, QUEST, 8, 128), bf16),
        vmem((NZ * QUEST * 8, 128), f32),
        dma((len(shards) + 6,)),
        dma((NZ,)),
        dma((2, NX // 2, NZ)),
        dma((NX,)),
        dma((2, NZ // 2, NX)),
        dma((6,)),
        dma((2,)),
        dma((2,)),
        dma((chunks,)),
        dma((chunks,)),
        dma((NZ,)),
        dma((NZ,)),
        dma((NX,)),
        dma((NZ,)),
        dma((1,)),
        dma((NZ,)),
        dma((NZ,)),
        dma((1,)),
        dma((1,)),
        dma((NX,)),
        dma((NZ,)),
    ]
    return pl.pallas_call(
        reader_kernel,
        out_shape=(
            jax.ShapeDtypeStruct((rows, width), bf16),
            jax.ShapeDtypeStruct((QUEST * answers, half), bf16),
        ),
        in_specs=[pl.BlockSpec(memory_space=pl.ANY)] * 13
        + [pl.BlockSpec(memory_space=pltpu.SMEM)],
        out_specs=(pl.BlockSpec(memory_space=pl.ANY), pl.BlockSpec(memory_space=vmem)),
        scratch_shapes=scratch,
        compiler_params=pltpu.CompilerParams(
            collective_id=1, has_side_effects=True, vmem_limit_bytes=60 * 2**20
        ),
        name="reader",
    )(hidden, *gains, *shards, table, ids, lengths)


def per_device(
    hidden_in,
    ffn_gain,
    wi_gate,
    wi_up,
    wo_down,
    final_gain,
    key_w,
    value_w,
    query_w,
    out_w,
    dec_gain,
    embed,
    lengths,
    answer_ids,
):
    gains = (ffn_gain, final_gain, dec_gain)
    shards = (wi_gate, wi_up, wo_down.T, key_w, value_w, query_w, out_w.T)
    return reader(hidden_in, gains, shards, embed, answer_ids, lengths)


def solution(mesh):
    torus = Mesh(
        mesh.devices.reshape(mesh.shape["groups"], NX, NZ, mesh.shape["narrow"]),
        ("groups", "wide_0", "wide_1", "narrow"),
    )
    return jax.shard_map(
        per_device,
        mesh=torus,
        in_specs=(
            P(GROUPS_WIDE, None),
            P(),
            P(WIDE, "narrow"),
            P(WIDE, "narrow"),
            P("narrow", WIDE),
            P(),
            P(WIDE, "narrow"),
            P(WIDE, "narrow"),
            P(WIDE, "narrow"),
            P("narrow", WIDE),
            P(),
            P(WIDE, None),
            P(GROUPS_WIDE),
            P("groups", None),
        ),
        out_specs=(P(GROUPS_WIDE, None), P("groups", "narrow")),
        check_vma=False,
    )
```

```python
import functools
import math

import jax
import jax.numpy as jnp
from jax import lax
from jax.experimental import pallas as pl
from jax.experimental.pallas import tpu as pltpu
from jax.sharding import Mesh
from jax.sharding import PartitionSpec as P

HEAD_DIM = 64
QUEST = 4
WIDE = ("wide_0", "wide_1")
GROUPS_WIDE = ("groups", "wide_0", "wide_1")
X, Z, CORE = "wide_0", "wide_1", "narrow"
NX, NZ = 8, 16
MESH = pl.DeviceIdType.MESH

EPS = 1e-06
FLOOR = -1e30


def turn(i, by, n):
    return lax.rem(i + (by + 2 * n), n)


def others(axis, n, steps=None):
    me = lax.axis_index(axis)
    return [{axis: turn(me, d, n)} for d in (steps or range(1, n))]


def remote(src, dst, send, recv, peer):
    return pltpu.make_async_remote_copy(
        src_ref=src, dst_ref=dst, send_sem=send, recv_sem=recv, device_id=peer, device_id_type=MESH
    )


def join(parts):
    top = functools.reduce(jnp.maximum, [lse for _, lse in parts])
    weight, total = 0.0, 0.0
    for value, lse in parts:
        factor = jnp.exp(lse - top)
        weight = weight + factor
        total = total + factor * value
    return total / weight, top + jnp.log(weight)


def dot(a, b, transposed=False):
    return lax.dot_general(
        a, b, (((1,), (1 if transposed else 0,)), ((), ())), preferred_element_type=jnp.float32
    )


def gain_of(ref):
    return ref[...].astype(jnp.float32).reshape(1, -1)


def rows_of(index, count):
    return pl.ds(pl.multiple_of(index * count, count), count)


def reader_kernel(
    hidden_in,
    ffn_gain_in,
    final_gain_in,
    dec_gain_in,
    gate_w,
    up_w,
    down_w,
    key_w,
    value_w,
    query_w,
    out_w,
    table_in,
    ids_in,
    lengths,
    memory_out,
    decoded,
    hidden,
    ffn_gain,
    final_gain,
    dec_gain,
    table,
    ids,
    memory,
    spread_picks,
    a_own,
    b_own,
    fa,
    fb,
    enc,
    inner,
    down_mine,
    down_other,
    picks,
    e1,
    e2_src,
    e2,
    e3_src,
    e3,
    e4,
    emb,
    own_rows,
    part,
    f1,
    f2_src,
    f2,
    wide,
    f3_src,
    f3,
    f4_src,
    f4,
    f5,
    flat,
    load_sem,
    a1,
    a2,
    b1,
    b2,
    sends,
    y_send,
    y_recv,
    down_send,
    down_recv,
    e_send,
    e_r1,
    e_r2,
    e_r3,
    e_r4,
    f_send,
    f_r1,
    f_r2,
    f_r3,
    f_r4,
    f_r5,
):
    f32, bf16 = jnp.float32, jnp.bfloat16
    x, z, n = lax.axis_index(X), lax.axis_index(Z), lax.axis_index(CORE)
    core = {CORE: 1 - n}
    group = lax.axis_index("groups")
    parity = lax.rem(group, 2)
    partner = {"groups": group + 1 - 2 * parity}
    mate = x + 1 - 2 * lax.rem(x, 2)
    ff, proj = gate_w.shape[1], key_w.shape[1]
    width = hidden.shape[1]
    half = width // 2
    rows = hidden.shape[0]
    answers = own_rows.shape[0]
    loads, at = [], 0
    for ref in (down_w, key_w, value_w, query_w, out_w):
        loads.append((ref, a_own.at[:, at : at + ref.shape[1]]))
        at += ref.shape[1]
    loads += [(gate_w, b_own.at[:, :ff]), (up_w, b_own.at[:, ff:])]
    loads += [(ids_in, ids), (table_in.at[:, rows_of(n, half)], table)]
    shard_loads = len(loads)
    loads += [(hidden_in, hidden), (ffn_gain_in, ffn_gain)]
    loads += [(final_gain_in, final_gain), (dec_gain_in, dec_gain)]
    loads = [
        pltpu.make_async_copy(src, dst, load_sem.at[k]) for k, (src, dst) in enumerate(loads)
    ]
    for load in loads:
        load.start()
    peers = others(X, NX) + others(Z, NZ) + [core, partner]
    barrier = pltpu.get_barrier_semaphore()
    for peer in peers:
        pl.semaphore_signal(barrier, inc=1, device_id=peer, device_id_type=MESH)
    for load in loads[:shard_loads]:
        load.wait()

    vocab_rows = table.shape[0]
    spot = lax.broadcasted_iota(jnp.int32, (vocab_rows, answers), 0)
    for q in range(QUEST):
        local_ids = ids[q : q + 1] - (x * NZ + z) * vocab_rows
        shares = lax.dot_general(
            (spot == local_ids).astype(f32).astype(bf16),
            table[...],
            (((0,), (0,)), ((), ())),
            preferred_element_type=f32,
        )
        for i in range(2):
            for r in range(half // 128):
                spread_picks[r, pl.ds(2 * q + i, NZ, stride=NX), :] = shares[
                    NZ * i : NZ * (i + 1), 128 * r : 128 * (r + 1)
                ]
    for k in range(NZ):
        for r in range(half // 128):
            picks[k, :, 128 * r : 128 * (r + 1)] = spread_picks[
                r, NX * k : NX * (k + 1)
            ].astype(bf16)
    pl.semaphore_wait(barrier, len(peers))

    def block_a(first, second):
        return turn(x, second, NX) * NZ + turn(z, first, NZ)

    def block_b(first, second):
        return turn(x, first, NX) * NZ + turn(z, second, NZ)

    plans = []
    for index, (src, full, block, axis1, n1, axis2, n2, sem1, sem2) in enumerate(
        ((a_own, fa, block_a, Z, NZ, X, NX, a1, a2), (b_own, fb, block_b, X, NX, Z, NZ, b1, b2))
    ):
        total = src.shape[1]
        share = total // 128 * 2 // 9 * 128
        columns = total - share
        middle = columns // 256 * 128
        start = parity * share
        cuts = (
            pl.ds(pl.multiple_of(start, 128), middle),
            pl.ds(pl.multiple_of(start + middle, 128), columns - middle),
        )
        area = pl.ds(pl.multiple_of(start, 128), columns)
        given = pl.ds(pl.multiple_of(parity * columns, 128), share)
        me1, me2 = lax.axis_index(axis1), lax.axis_index(axis2)
        peers1 = tuple({axis1: turn(me1, d, n1)} for d in (1, -1))
        peers2 = tuple({axis2: turn(me2, d, n2)} for d in (1, -1))
        plans.append(
            (index, src, full, block, n1, n2, sem1, sem2, cuts, peers1, peers2, area, given)
        )

    def off(k):
        odd = lax.rem(k, 2)
        return (1 - odd) * (k // 2) - odd * ((k + 1) // 2)

    def hand_over(plan, src, which):
        index, full, given = plan[0], plan[2], plan[12]
        remote(
            src.at[:, given], full.at[which, :, given], y_send.at[index], y_recv.at[index], partner
        ).start()

    def first_stage(plan, t):
        index, src, full, block, n1, n2, sem1, sem2, cuts, peers1, peers2, area, given = plan
        send = sends.at[3 * index]

        @pl.when(t == 0)
        def _():
            mine = full.at[block(0, 0), :, area]
            hand_over(plan, src, block(0, 0))
            sent = src.at[:, area]
            for d in range(2):
                remote(sent, mine, send, sem1.at[1 + d], peers1[d]).start()
            for d in range(2):
                remote(sent, mine, send, sem2.at[d, 0, 0], peers2[d]).start()

        @pl.when((t > 0) & (t < n1))
        def _():
            at = full.at[block(off(t), 0), :, area]
            remote(at, at, send, sem1.at[t], peers1[0]).wait_recv()
            odd = lax.rem(t, 2)

            @pl.when((odd == 1) & (t < n1 - 1))
            def _():
                remote(at, at, send, sem1.at[t + 2], peers1[0]).start()

            @pl.when((odd == 0) & (t < n1 - 2))
            def _():
                remote(at, at, send, sem1.at[t + 2], peers1[1]).start()

            for d in range(2):
                remote(at, at, send, sem2.at[d, 0, t], peers2[d]).start()
            hand_over(plan, full.at[block(off(t), 0)], block(off(t), 0))

    def later_stage(plan, t, h):
        index, src, full, block, n1, n2, sem1, sem2, cuts, peers1, peers2, area, given = plan
        last = n2 // 2
        k = t - 2 * h

        @pl.when((k >= 0) & (k < n1))
        def _():
            for d in range(2):
                which = block(off(k), -h if d == 0 else h)
                at = full.at[which, :, area]
                part = full.at[which, :, cuts[d]]
                if h == last:
                    remote(
                        part, part, sends.at[3 * index + 1 + d], sem2.at[d, h - 1, k], peers2[d]
                    ).wait_recv()
                    if d == 1:
                        hand_over(plan, full.at[which], which)
                    continue
                remote(at, at, sends.at[3 * index], sem2.at[d, h - 1, k], peers2[d]).wait_recv()
                if h + 1 == last:
                    remote(
                        part, part, sends.at[3 * index + 1 + d], sem2.at[d, h, k], peers2[d]
                    ).start()
                else:
                    remote(at, at, sends.at[3 * index], sem2.at[d, h, k], peers2[d]).start()
                hand_over(plan, full.at[which], which)

    def tick(t, carry):
        for plan in plans:
            first_stage(plan, t)
        for h in range(1, max(NX, NZ) // 2 + 1):
            for plan in plans:
                if h <= plan[5] // 2:
                    later_stage(plan, t, h)
        return carry

    first_copies = []
    for d in range(1, NZ):
        to = turn(z, d, NZ)
        copy = remote(picks.at[to], e1.at[d], e_send.at[d], e_r1.at[d], {Z: to})
        copy.start()
        first_copies.append(copy)
    lax.fori_loop(0, 2, tick, 0)

    for load in loads[shard_loads:]:
        load.wait()
    resid_in = hidden[...].astype(f32)
    mean_square = jnp.mean(resid_in * resid_in, axis=-1, keepdims=True)
    enc[...] = (resid_in * lax.rsqrt(mean_square + EPS) * gain_of(ffn_gain)).astype(bf16)
    for index, src, full, block, *_, area, given in plans:
        full[block(0, 0), :, area] = src[:, area]
    lax.fori_loop(2, 5, tick, 0)

    total = picks[z].astype(f32)
    for d, copy in enumerate(first_copies, 1):
        copy.wait_recv()
        total = total + e1[d].astype(f32)
    for copy in first_copies:
        copy.wait_send()
    for q in range(QUEST):
        for r in range(half // 128):
            e2_src[q, 2 * r : 2 * r + 2] = total[2 * q : 2 * q + 2, 128 * r : 128 * (r + 1)]
    copies = []
    for d in range(1, NX):
        to = turn(x, d, NX)
        copy = remote(e2_src.at[to // 2], e2.at[d], e_send.at[d], e_r2.at[d], {X: to})
        copy.start()
        copies.append(copy)
    lax.fori_loop(5, 8, tick, 0)

    total = e2_src[x // 2]
    for d, copy in enumerate(copies, 1):
        copy.wait_recv()
        total = total + e2[d]
    for copy in copies:
        copy.wait_send()
    e3_src[...] = total.astype(bf16)
    e3[z] = total.astype(bf16)
    copies = []
    for d in range(1, NZ):
        copy = remote(e3_src, e3.at[z], e_send.at[d], e_r3.at[d], {Z: turn(z, d, NZ)})
        copy.start()
        copies.append(copy)
    lax.fori_loop(8, 12, tick, 0)

    for d in range(1, NZ):
        slot = e3.at[turn(z, -d, NZ)]
        remote(slot, slot, e_send.at[d], e_r3.at[d], {Z: turn(z, d, NZ)}).wait_recv()
    for copy in copies:
        copy.wait_send()
    copy = remote(e3, e4.at[n], e_send.at[0], e_r4.at[0], core)
    copy.start()
    e4[n] = e3[...]
    lax.fori_loop(12, 16, tick, 0)

    slot = e4.at[1 - n]
    remote(slot, slot, e_send.at[0], e_r4.at[0], core).wait_recv()
    copy.wait_send()
    emb[...] = e4[...].astype(f32).reshape(emb.shape)
    for h in range(2):
        for r in range(half // 128):
            for i in range(2):
                own_rows[NZ * i : NZ * (i + 1), half * h + 128 * r : half * h + 128 * (r + 1)] = (
                    emb[pl.ds(8 * NZ * h + 2 * r + i, NZ, stride=8), :]
                )
    embedded = own_rows[...]
    mean_square = jnp.mean(embedded * embedded, axis=-1, keepdims=True)
    dec_in = (embedded * lax.rsqrt(mean_square + EPS) * gain_of(dec_gain)).astype(bf16)
    lax.fori_loop(16, NX + NZ, tick, 0)

    for index, src, full, block, n1, n2, sem1, sem2, cuts, peers1, peers2, area, given in plans:
        count = (n1 - 1) + 2 * n1 * (n2 // 2 - 1)
        whole = full.at[:, :, given]
        remote(whole, whole, y_send.at[index], y_recv.at[index], partner).wait()
        whole = full.at[pl.ds(0, count), :, area]
        remote(whole, whole, sends.at[3 * index], sem1.at[0], peers1[0]).wait_send()
        for d in range(2):
            piece = full.at[pl.ds(0, n1), :, cuts[d]]
            remote(piece, piece, sends.at[3 * index + 1 + d], sem1.at[0], peers1[0]).wait_send()

    def ffn(c, carry):
        gate_at = pl.ds(pl.multiple_of(c * 128, 128), 128)
        up_at = pl.ds(pl.multiple_of(ff + c * 128, 128), 128)
        weight = jnp.concatenate((fb[:, :, gate_at], fb[:, :, up_at]), axis=2).reshape(width, 256)
        both = dot(enc[...], weight)
        value = jax.nn.gelu(both[:, :128], approximate=True) * both[:, 128:]
        inner[:, rows_of(c, 128)] = value.astype(bf16)
        return carry

    lax.fori_loop(0, ff // 128, ffn, 0)
    copies = []
    for c in range(width // 256):
        weight = fa[32 * c : 32 * (c + 1), :, :ff].reshape(256, ff)
        down_mine[c] = dot(inner[...], weight, True)
        copy = remote(down_mine.at[c], down_other.at[c], down_send.at[c], down_recv.at[c], core)
        copy.start()
        copies.append(copy)
    query = dot(dec_in, fa[:, :, ff + 2 * proj : ff + 3 * proj].reshape(width, proj)).astype(bf16)
    squares = 0.0
    for c, copy in enumerate(copies):
        copy.wait_recv()
        resid = hidden[:, 256 * c : 256 * (c + 1)].astype(f32) + (down_mine[c] + down_other[c])
        down_other[c] = resid
        squares = squares + jnp.sum(resid * resid, axis=-1, keepdims=True)
    scale = lax.rsqrt(squares * (1.0 / width) + EPS)
    gain = gain_of(final_gain)
    for c in range(width // 256):
        cols = slice(256 * c, 256 * (c + 1))
        memory[:, cols] = (down_other[c] * scale * gain[:, cols]).astype(bf16)
    for copy in copies:
        copy.wait_send()
    store = pltpu.make_async_copy(memory, memory_out, load_sem.at[0])
    store.start()

    mem = memory[...]
    keys = dot(mem, fa[:, :, ff : ff + proj].reshape(width, proj)).astype(bf16)
    values = dot(mem, fa[:, :, ff + proj : ff + 2 * proj].reshape(width, proj)).astype(bf16)
    heads = proj // HEAD_DIM
    head_of = lax.broadcasted_iota(jnp.int32, (answers, proj), 1) // HEAD_DIM
    spread = jnp.concatenate(
        [jnp.where(head_of == h, query.astype(f32), 0.0) for h in range(heads)], axis=0
    ).astype(bf16)
    scores = dot(spread, keys, True) * (1.0 / math.sqrt(HEAD_DIM))
    position = lax.broadcasted_iota(jnp.int32, scores.shape, 1)
    passages = lengths.shape[0]
    passage_len = rows // passages
    live = None
    for p in range(passages):
        here = (position >= p * passage_len) & (position < p * passage_len + lengths[p])
        live = here if live is None else live | here
    scores = jnp.where(live, scores, FLOOR)
    top = jnp.max(scores, axis=1, keepdims=True)
    weights = jnp.exp(scores - top)
    total = jnp.sum(weights, axis=1, keepdims=True)
    acc = dot(weights.astype(bf16), values) / total
    lse = top + jnp.log(total)
    value, spread_lse = 0.0, 0.0
    for h in range(heads):
        rows_h = slice(answers * h, answers * (h + 1))
        value = value + jnp.where(head_of == h, acc[rows_h], 0.0)
        spread_lse = spread_lse + jnp.where(head_of == h, lse[rows_h], 0.0)
    for s, block_of in enumerate((value, spread_lse)):
        for r in range(proj // 128):
            for i in range(2):
                part[pl.ds(8 * s + 2 * r + i, NZ, stride=16), :] = block_of[
                    NZ * i : NZ * (i + 1), 128 * r : 128 * (r + 1)
                ]

    copies = []
    for d in range(1, NZ):
        to = turn(z, d, NZ)
        copy = remote(
            part.at[rows_of(to, 16)], f1.at[d], f_send.at[d], f_r1.at[d], {Z: to}
        )
        copy.start()
        copies.append(copy)
    mine = part[rows_of(z, 16)]
    parts = [(mine[:8], mine[8:])]
    for d, copy in enumerate(copies, 1):
        copy.wait_recv()
        parts.append((f1[d, :8], f1[d, 8:]))
    value, lse = join(parts)
    f2_src[0] = value
    f2_src[1] = lse
    pair = remote(f2_src, f2, f_send.at[0], f_r2.at[0], {X: mate})
    pair.start()
    for copy in copies:
        copy.wait_send()
    pair.wait()
    value, _ = join([(value, lse), (f2[0], f2[1])])
    wide[...] = value
    slices = proj // 128
    summed = 0.0
    for r in range(slices):
        lhs = wide[2 * r : 2 * r + 2].astype(bf16)
        at = ff + 3 * proj + 128 * r
        summed = summed + dot(lhs, fa[:, :, at : at + 128].reshape(width, 128), True)
    for h in range(2):
        for r in range(half // 128):
            at = half * h + 128 * r
            f3_src[h, 2 * r : 2 * r + 2] = summed[:, at : at + 128]
    copy = remote(f3_src.at[1 - n], f3, f_send.at[0], f_r3.at[0], core)
    copy.start()
    copy.wait()
    result = emb[pl.ds(pl.multiple_of(n * 8 * NZ + z * 8, 8), 8)] + (f3_src[n] + f3[...])
    done = result.astype(bf16)
    f4_src[...] = done
    f4[x // 2] = done
    copies = []
    for d in (2, 4, 6):
        copy = remote(f4_src, f4.at[x // 2], f_send.at[d], f_r4.at[d], {X: turn(x, d, NX)})
        copy.start()
        copies.append(copy)
    for d in (2, 4, 6):
        slot = f4.at[turn(x, -d, NX) // 2]
        remote(slot, slot, f_send.at[d], f_r4.at[d], {X: turn(x, d, NX)}).wait_recv()
    for copy in copies:
        copy.wait_send()
    copies = []
    for d in range(1, NZ):
        copy = remote(f4, f5.at[z], f_send.at[d], f_r5.at[d], {Z: turn(z, d, NZ)})
        copy.start()
        copies.append(copy)
    f5[z] = f4[...]
    for d in range(1, NZ):
        slot = f5.at[turn(z, -d, NZ)]
        remote(slot, slot, f_send.at[d], f_r5.at[d], {Z: turn(z, d, NZ)}).wait_recv()
    for k in range(NZ):
        for q in range(QUEST):
            flat[8 * (QUEST * k + q) : 8 * (QUEST * k + q + 1)] = f5[k, q].astype(f32)
    for q in range(QUEST):
        for i in range(2):
            for r in range(half // 128):
                start = NZ * (2 * q + i)
                decoded[start : start + NZ, 128 * r : 128 * (r + 1)] = flat[
                    pl.ds(8 * q + 2 * r + i, NZ, stride=8 * QUEST), :
                ].astype(bf16)
    for copy in copies:
        copy.wait_send()
    store.wait()


def reader(hidden, gains, shards, table, ids, lengths):
    gate_w, up_w, down_w, key_w, value_w, query_w, out_w = shards
    dma = pltpu.SemaphoreType.DMA
    f32, bf16 = jnp.float32, jnp.bfloat16
    blocks = NX * NZ
    answers = ids.shape[1]
    rows, width = hidden.shape
    ff, proj, half = gate_w.shape[1], key_w.shape[1], width // 2
    a_width, b_width = ff + 4 * proj, 2 * ff
    chunks = width // 256
    vmem = pltpu.VMEM
    scratch = [
        vmem((rows, width), bf16),
        *[vmem(gain.shape, bf16) for gain in gains],
        vmem((table.shape[0], half), bf16),
        vmem(ids.shape, ids.dtype),
        vmem((rows, width), bf16),
        vmem((half // 128, NX * NZ, 128), f32),
        vmem((8, a_width), bf16),
        vmem((8, b_width), bf16),
        vmem((blocks, 8, a_width), bf16),
        vmem((blocks, 8, b_width), bf16),
        vmem((rows, width), bf16),
        vmem((rows, ff), bf16),
        vmem((chunks, rows, 256), f32),
        vmem((chunks, rows, 256), f32),
        vmem((NZ, NX, half), bf16),
        vmem((NZ, NX, half), bf16),
        vmem((QUEST, 8, 128), f32),
        vmem((NX, 8, 128), f32),
        vmem((8, 128), bf16),
        vmem((NZ, 8, 128), bf16),
        vmem((2, NZ, 8, 128), bf16),
        vmem((16 * NZ, 128), f32),
        vmem((answers, width), f32),
        vmem((16 * NZ, 128), f32),
        vmem((NZ, 16, 128), f32),
        vmem((2, 8, 128), f32),
        vmem((2, 8, 128), f32),
        vmem((8, 128), f32),
        vmem((2, 8, 128), f32),
        vmem((8, 128), f32),
        vmem((8, 128), bf16),
        vmem((QUEST, 8, 128), bf16),
        vmem((NZ, QUEST, 8, 128), bf16),
        vmem((NZ * QUEST * 8, 128), f32),
        dma((len(shards) + 6,)),
        dma((NZ,)),
        dma((2, NX // 2, NZ)),
        dma((NX,)),
        dma((2, NZ // 2, NX)),
        dma((6,)),
        dma((2,)),
        dma((2,)),
        dma((chunks,)),
        dma((chunks,)),
        dma((NZ,)),
        dma((NZ,)),
        dma((NX,)),
        dma((NZ,)),
        dma((1,)),
        dma((NZ,)),
        dma((NZ,)),
        dma((1,)),
        dma((1,)),
        dma((NX,)),
        dma((NZ,)),
    ]
    return pl.pallas_call(
        reader_kernel,
        out_shape=(
            jax.ShapeDtypeStruct((rows, width), bf16),
            jax.ShapeDtypeStruct((QUEST * answers, half), bf16),
        ),
        in_specs=[pl.BlockSpec(memory_space=pl.ANY)] * 13
        + [pl.BlockSpec(memory_space=pltpu.SMEM)],
        out_specs=(pl.BlockSpec(memory_space=pl.ANY), pl.BlockSpec(memory_space=vmem)),
        scratch_shapes=scratch,
        compiler_params=pltpu.CompilerParams(
            collective_id=1, has_side_effects=True, vmem_limit_bytes=60 * 2**20
        ),
        name="reader",
    )(hidden, *gains, *shards, table, ids, lengths)


def per_device(
    hidden_in,
    ffn_gain,
    wi_gate,
    wi_up,
    wo_down,
    final_gain,
    key_w,
    value_w,
    query_w,
    out_w,
    dec_gain,
    embed,
    lengths,
    answer_ids,
):
    gains = (ffn_gain, final_gain, dec_gain)
    shards = (wi_gate, wi_up, wo_down.T, key_w, value_w, query_w, out_w.T)
    return reader(hidden_in, gains, shards, embed, answer_ids, lengths)


def solution(mesh):
    torus = Mesh(
        mesh.devices.reshape(mesh.shape["groups"], NX, NZ, mesh.shape["narrow"]),
        ("groups", "wide_0", "wide_1", "narrow"),
    )
    return jax.shard_map(
        per_device,
        mesh=torus,
        in_specs=(
            P(GROUPS_WIDE, None),
            P(),
            P(WIDE, "narrow"),
            P(WIDE, "narrow"),
            P("narrow", WIDE),
            P(),
            P(WIDE, "narrow"),
            P(WIDE, "narrow"),
            P(WIDE, "narrow"),
            P("narrow", WIDE),
            P(),
            P(WIDE, None),
            P(GROUPS_WIDE),
            P("groups", None),
        ),
        out_specs=(P(GROUPS_WIDE, None), P("groups", "narrow")),
        check_vma=False,
    )
```
